128 devices in a mesh: band: 16 (over x, y), tm: 8 (over z, core).
Axes of the slice: x: 4, y: 4, z: 4, core: 2. Of those that a mesh axis runs over, the one named last changes fastest.
Arguments:
- spec: bfloat16 [2048, 4096], P('tm', 'band'), may hold values from -6 to 6
- cotangent: bfloat16 [2048, 4096], P('tm', 'band'), may hold values from -0.29882812 to 0.29882812
- widths: int32 [32], replicated, may hold values from 16 to 64, as said below
- band_group: int32 [32], replicated, may hold values from 0 to 15, as said below
- w_embed: bfloat16 [256, 64, 384], P(None, 'band'), may hold values from -0.375 to 0.375
- w_qkv: bfloat16 [384, 1536], replicated, may hold values from -2 to 2
- w_proj: bfloat16 [512, 384], replicated, may hold values from -0.25 to 0.25
- w_hidden: bfloat16 [384, 64, 1536], P(None, 'band'), may hold values from -0.3125 to 0.3125
- w_out: bfloat16 [1536, 64, 512], P(None, 'band'), may hold values from -0.15625 to 0.15625
Outputs:
- mask: bfloat16 [2048, 4096], P('tm', 'band')
- grad_embed: bfloat16 [256, 64, 384], P('tm', 'band')
- grad_qkv: float32 [384, 1536], replicated
- grad_proj: float32 [512, 384], replicated
- grad_hidden: bfloat16 [384, 64, 1536], P('tm', 'band')
- grad_out: bfloat16 [1536, 64, 512], P('tm', 'band')
The draws below stay inside these ranges and needn't reach their ends.
Inputs may be any that keep to these rules, and one draw needn't show every extreme that they name: The widths sum to 1024 and at least one band has exactly 64 bins. `band_group`: every group owns at most 4 bands, and some group owns exactly 4.
All inputs are finite; a program needn't handle non-finite values.
Results may differ from the reference program's by a relative error of at most 0.02.
Values may be sent and summed in bfloat16 or wider, within the bound.
A program may use at most 128 MiB of HBM per device.

```python
import jax
import jax.numpy as jnp
from jax import lax

D = 384
HEADS = 8
HEAD_DIM = 64
MLP_WIDTH = 1536
BANDS = 32
FREQ = 1024
WPAD = 64
FRAMES_DEV = 256
FRAMES = 2048
SLOTS = 4
N_BAND = 16
N_TM = 8


def draw_widths(key, part):
    lowest = WPAD // 4
    spare_room = WPAD - lowest
    surplus = FREQ - BANDS * lowest
    positions = jnp.arange(BANDS)
    filled = (surplus // BANDS + jnp.where(positions < surplus % BANDS, 1, 0)).astype(jnp.int32)

    def transfer(iteration, values):
        step_key = jax.random.fold_in(key, iteration)
        key_source, key_target, key_amount = jax.random.split(step_key, 3)
        source = jax.random.randint(key_source, (), 0, BANDS)
        target = jax.random.randint(key_target, (), 0, BANDS)
        ceiling = jnp.minimum(values[source], spare_room - values[target])
        amount = jax.random.randint(key_amount, (), 0, ceiling + 1)
        amount = jnp.where(source == target, 0, amount)
        return values.at[source].add(-amount).at[target].add(amount)
    values = lax.fori_loop(0, 8 * BANDS, transfer, filled)
    chosen = jax.random.randint(jax.random.fold_in(key, 100003), (), 0, BANDS)

    def top_up(donating, values):
        needed = spare_room - values[chosen]
        moved_amount = jnp.where(donating == chosen, 0, jnp.minimum(needed, values[donating]))
        return values.at[donating].add(-moved_amount).at[chosen].add(moved_amount)
    values = lax.fori_loop(0, BANDS, top_up, values)
    return (values + lowest).astype(jnp.int32)


def draw_band_group(key, part):
    key_full, key_order, key_rest = jax.random.split(jax.random.fold_in(key, 7), 3)
    fullest = jax.random.randint(key_full, (), 0, N_BAND)
    shuffled = jax.random.permutation(key_order, BANDS)
    others = jax.random.permutation(key_rest, (N_BAND - 1) * SLOTS) // SLOTS
    others = others + jnp.where(others >= fullest, 1, 0)
    positions = jnp.arange(BANDS)
    picked = jnp.where(positions < SLOTS, fullest, others[jnp.maximum(positions - SLOTS, 0)])
    return jnp.zeros((BANDS,), jnp.int32).at[shuffled].set(picked.astype(jnp.int32))


def draw_w_qkv(key, part):
    inner_width = HEADS * HEAD_DIM
    key_base = jax.random.fold_in(jax.random.fold_in(key, 11), 0)
    base = jax.random.normal(key_base, (D, 3 * inner_width), jnp.float32) * D ** (-0.5)
    result = base
    result = jnp.clip(result, -2.0, 2.0)
    return result.astype(jnp.bfloat16)


def block_levels(rng, shape, cuts, least, top_value):
    level = 1.0
    for dim, shards_of in cuts:
        heights = jax.random.uniform(jax.random.fold_in(jax.random.fold_in(rng, 6), dim), (shards_of,), jnp.float32, least / len(cuts), top_value / len(cuts))
        level = level * jnp.repeat(jnp.exp(heights), shape[dim] // shards_of).reshape((-1,) + (1,) * (len(shape) - 1 - dim))
    return level


def centred(rng, extent, deviation, reach, cuts=(), kind=jnp.bfloat16):
    factor_of = block_levels(rng, extent, cuts, -0.22, 0.18) if cuts else 1.0
    entries = jax.random.normal(rng, extent, jnp.float32) * deviation * factor_of
    return jnp.minimum(jnp.maximum(entries, -reach), reach).astype(kind)


def setup_inputs(seed: int = 0) -> dict:
    arg_keys = jax.random.split(jax.random.key(seed), 10)
    spec = centred(arg_keys[0], (FRAMES, 4 * FREQ), 1.0, 6.0, ((0, 8), (1, 16)))
    cotangent = centred(arg_keys[1], (FRAMES, 4 * FREQ), 0.05, 0.29882812, ((0, 8), (1, 16)))
    widths = draw_widths(jax.random.fold_in(arg_keys[9], 71), 0)
    band_group = draw_band_group(jax.random.fold_in(arg_keys[9], 71), 0)
    w_embed = centred(arg_keys[4], (4 * WPAD, N_BAND * SLOTS, D), (4 * WPAD) ** -0.5, 0.375, ((1, 16),))
    w_qkv = draw_w_qkv(jax.random.fold_in(arg_keys[9], 71), 0)
    w_proj = centred(arg_keys[6], (HEADS * HEAD_DIM, D), (HEADS * HEAD_DIM) ** -0.5, 0.25)
    w_hidden = centred(arg_keys[7], (D, N_BAND * SLOTS, MLP_WIDTH), D ** -0.5, 0.3125, ((1, 16),))
    w_out = centred(arg_keys[8], (MLP_WIDTH, N_BAND * SLOTS, 8 * WPAD), MLP_WIDTH ** -0.5, 0.15625, ((1, 16),))
    return dict(spec=spec, cotangent=cotangent, widths=widths, band_group=band_group, w_embed=w_embed, w_qkv=w_qkv, w_proj=w_proj, w_hidden=w_hidden, w_out=w_out)


EPSILON = 1e-05

def row_norm(values):
    inv_rms = lax.rsqrt(lax.optimization_barrier(jnp.mean(values * values, axis=-1, keepdims=True)) + EPSILON)
    return (values * inv_rms, inv_rms)

def attention_forward(tokens, w_qkv, w_proj):
    inner_width = w_proj.shape[0]
    head_count = inner_width // HEAD_DIM
    rows, width_k = (tokens.shape[0], tokens.shape[1])
    token32 = tokens.astype(jnp.float32)
    normed32, inv_rms = row_norm(token32)
    normed = normed32.astype(jnp.bfloat16)
    packed = jnp.einsum('nkd,de->nke', normed.astype(jnp.float32), w_qkv.astype(jnp.float32)).astype(jnp.bfloat16)
    queries = packed[:, :, :inner_width].reshape(rows, width_k, head_count, HEAD_DIM)
    key_rows = packed[:, :, inner_width:2 * inner_width].reshape(rows, width_k, head_count, HEAD_DIM)
    value_rows = packed[:, :, 2 * inner_width:].reshape(rows, width_k, head_count, HEAD_DIM)
    scores = jnp.einsum('nqhc,nkhc->nhqk', queries.astype(jnp.float32), key_rows.astype(jnp.float32)) * HEAD_DIM ** (-0.5)
    highest = lax.optimization_barrier(jnp.max(scores, axis=-1, keepdims=True))
    expd = jnp.exp(scores - highest)
    soft_weights = expd / lax.optimization_barrier(jnp.sum(expd, axis=-1, keepdims=True))
    soft_rounded = soft_weights.astype(jnp.bfloat16)
    heads_out = jnp.einsum('nhqk,nkhc->nqhc', soft_rounded.astype(jnp.float32), value_rows.astype(jnp.float32))
    heads_out = heads_out.astype(jnp.bfloat16).reshape(rows, width_k, inner_width)
    result = token32 + jnp.einsum('nki,id->nkd', heads_out.astype(jnp.float32), w_proj.astype(jnp.float32))
    saved = (normed32, inv_rms, normed, queries, key_rows, value_rows, soft_weights, soft_rounded, heads_out)
    return (result.astype(jnp.bfloat16), saved)

def attention_backward(saved, grad_out, w_qkv, w_proj):
    normed32, inv_rms, normed, queries, key_rows, value_rows, soft_weights, soft_rounded, heads_out = saved
    inner_width = w_proj.shape[0]
    head_count = inner_width // HEAD_DIM
    rows, width_k = (grad_out.shape[0], grad_out.shape[1])
    grad32 = grad_out.astype(jnp.float32)
    grad_proj = jnp.einsum('nki,nkd->id', heads_out.astype(jnp.float32), grad32)
    grad_heads = jnp.einsum('nkd,id->nki', grad32, w_proj.astype(jnp.float32)).astype(jnp.bfloat16)
    grad_heads = grad_heads.reshape(rows, width_k, head_count, HEAD_DIM).astype(jnp.float32)
    grad_soft = jnp.einsum('nqhc,nkhc->nhqk', grad_heads, value_rows.astype(jnp.float32))
    grad_values = jnp.einsum('nhqk,nqhc->nkhc', soft_rounded.astype(jnp.float32), grad_heads)
    grad_scores = soft_weights * (grad_soft - lax.optimization_barrier(jnp.sum(grad_soft * soft_weights, axis=-1, keepdims=True)))
    grad_scores = (grad_scores * HEAD_DIM ** (-0.5)).astype(jnp.bfloat16).astype(jnp.float32)
    grad_queries = jnp.einsum('nhqk,nkhc->nqhc', grad_scores, key_rows.astype(jnp.float32))
    grad_keys = jnp.einsum('nhqk,nqhc->nkhc', grad_scores, queries.astype(jnp.float32))
    grad_packed = jnp.concatenate([grad_queries.reshape(rows, width_k, inner_width), grad_keys.reshape(rows, width_k, inner_width), grad_values.reshape(rows, width_k, inner_width)], axis=-1).astype(jnp.bfloat16).astype(jnp.float32)
    grad_qkv = jnp.einsum('nkd,nke->de', normed.astype(jnp.float32), grad_packed)
    grad_normed = jnp.einsum('nke,de->nkd', grad_packed, w_qkv.astype(jnp.float32))
    grad_tokens = grad32 + inv_rms * (grad_normed - normed32 * lax.optimization_barrier(jnp.mean(grad_normed * normed32, axis=-1, keepdims=True)))
    return (grad_tokens.astype(jnp.bfloat16), grad_qkv, grad_proj)

def block_grad(left, right):
    left_blocks = left.reshape(N_TM, FRAMES_DEV, left.shape[1]).astype(jnp.float32)
    right_blocks = right.reshape(N_TM, FRAMES_DEV, right.shape[1]).astype(jnp.float32)
    partial_sums = jnp.einsum('nfa,nfb->nab', left_blocks, right_blocks).astype(jnp.bfloat16)
    partial_sums = lax.optimization_barrier(partial_sums)
    return lax.optimization_barrier(jnp.sum(partial_sums.astype(jnp.float32), axis=0))

def band_tail(mixed_band, cot_tile, valid, w_hid, w_output):
    feat = cot_tile.shape[1]
    mixed32 = mixed_band.astype(jnp.float32)
    normed32, inv_rms = row_norm(mixed32)
    normed = normed32.astype(jnp.bfloat16)
    pre_act = jnp.dot(normed, w_hid, preferred_element_type=jnp.float32)
    tanh_act = jnp.tanh(pre_act)
    hidden_act = tanh_act.astype(jnp.bfloat16)
    output = jnp.dot(hidden_act, w_output, preferred_element_type=jnp.float32)
    value_part = output[:, :feat]
    gate_part = jax.nn.sigmoid(output[:, feat:])
    band_mask = jnp.where(valid[None, :], value_part * gate_part, 0.0)
    grad_mask = jnp.where(valid[None, :], cot_tile.astype(jnp.float32), 0.0)
    grad_value = grad_mask * gate_part
    grad_gate = grad_mask * value_part * gate_part * (1.0 - gate_part)
    grad_output = jnp.concatenate([grad_value, grad_gate], axis=-1).astype(jnp.bfloat16)
    grad_act = jnp.dot(grad_output, w_output.T, preferred_element_type=jnp.float32)
    grad_pre = (grad_act * (1.0 - tanh_act * tanh_act)).astype(jnp.bfloat16)
    grad_normed = jnp.dot(grad_pre, w_hid.T, preferred_element_type=jnp.float32)
    grad_mixed = inv_rms * (grad_normed - normed32 * lax.optimization_barrier(jnp.mean(grad_normed * normed32, axis=-1, keepdims=True)))
    return (band_mask, grad_mixed.astype(jnp.bfloat16), block_grad(normed, grad_pre), block_grad(hidden_act, grad_output))

def reference(spec, cotangent, widths, band_group, w_embed, w_qkv, w_proj, w_hidden, w_out):
    feat = 4 * WPAD
    slot_count = N_BAND * SLOTS
    starts = (jnp.cumsum(widths) - widths).astype(jnp.int32)
    positions = jnp.arange(BANDS).astype(jnp.int32)
    same_group = band_group[:, None] == band_group[None, :]
    earlier = positions[None, :] < positions[:, None]
    ranks = lax.optimization_barrier(jnp.sum(jnp.where(same_group & earlier, 1, 0), axis=1)).astype(jnp.int32)
    slot_of = (band_group * SLOTS + ranks).astype(jnp.int32)
    spec_pad = jnp.pad(spec, ((0, 0), (0, feat)))
    cot_pad = jnp.pad(cotangent, ((0, 0), (0, feat)))
    lanes = jnp.arange(feat).astype(jnp.int32)

    def front(band_id):
        raw_bins = lax.dynamic_slice_in_dim(spec_pad, 4 * starts[band_id], feat, 1).astype(jnp.float32)
        valid = lanes < 4 * widths[band_id]
        raw_bins = jnp.where(valid[None, :], raw_bins, 0.0)
        square_mean = lax.optimization_barrier(jnp.sum(raw_bins * raw_bins, axis=-1, keepdims=True)) / (4 * widths[band_id]).astype(jnp.float32)
        normed = (raw_bins * lax.rsqrt(square_mean + EPSILON)).astype(jnp.bfloat16)
        weight = lax.dynamic_index_in_dim(w_embed, slot_of[band_id], 1, keepdims=False)
        return (normed, jnp.dot(normed, weight, preferred_element_type=jnp.float32).astype(jnp.bfloat16))
    band_normed, embedded = lax.map(front, positions)
    token_blocks = embedded.transpose(1, 0, 2).reshape(N_TM, FRAMES_DEV, BANDS, D)

    def forward_block(block_tokens):
        return attention_forward(block_tokens, w_qkv, w_proj)[0]
    mixed = lax.map(forward_block, token_blocks).reshape(FRAMES, BANDS, D)

    def tail(band_id):
        cot_tile = lax.dynamic_slice_in_dim(cot_pad, 4 * starts[band_id], feat, 1)
        valid = lanes < 4 * widths[band_id]
        w_hid = lax.dynamic_index_in_dim(w_hidden, slot_of[band_id], 1, keepdims=False)
        w_output = lax.dynamic_index_in_dim(w_out, slot_of[band_id], 1, keepdims=False)
        mixed_band = lax.dynamic_index_in_dim(mixed, band_id, 1, keepdims=False)
        return band_tail(mixed_band, cot_tile, valid, w_hid, w_output)
    mask_tiles, grad_mixed, grad_hid_bands, grad_out_bands = lax.map(tail, positions)

    def place(band_id, assembled):
        offset = 4 * starts[band_id]
        current = lax.dynamic_slice_in_dim(assembled, offset, feat, 1)
        return lax.dynamic_update_slice_in_dim(assembled, current + mask_tiles[band_id], offset, 1)
    assembled = lax.fori_loop(0, BANDS, place, jnp.zeros((FRAMES, 4 * FREQ + feat), jnp.float32))
    mask = assembled[:, :4 * FREQ].astype(jnp.bfloat16)
    grad_blocks = grad_mixed.transpose(1, 0, 2).reshape(N_TM, FRAMES_DEV, BANDS, D)

    def backward_block(pair):
        block_tokens, block_grads = pair
        unused_out, saved = attention_forward(block_tokens, w_qkv, w_proj)
        return attention_backward(saved, block_grads, w_qkv, w_proj)
    grad_tokens, grad_qkv_blocks, grad_proj_blocks = lax.map(backward_block, (token_blocks, grad_blocks))
    grad_qkv = lax.optimization_barrier(jnp.sum(grad_qkv_blocks, axis=0))
    grad_proj = lax.optimization_barrier(jnp.sum(grad_proj_blocks, axis=0))
    grad_embedded = grad_tokens.reshape(FRAMES, BANDS, D)

    def embed_grad(band_id):
        return block_grad(band_normed[band_id], lax.dynamic_index_in_dim(grad_embedded, band_id, 1, keepdims=False))
    grad_embed_bands = lax.map(embed_grad, positions)
    grad_embed = jnp.zeros((feat, slot_count, D), jnp.float32).at[:, slot_of, :].set(grad_embed_bands.transpose(1, 0, 2))
    grad_hidden = jnp.zeros((D, slot_count, MLP_WIDTH), jnp.float32).at[:, slot_of, :].set(grad_hid_bands.transpose(1, 0, 2))
    grad_out = jnp.zeros((MLP_WIDTH, slot_count, 2 * feat), jnp.float32).at[:, slot_of, :].set(grad_out_bands.transpose(1, 0, 2))
    return (mask, grad_embed.astype(jnp.bfloat16), grad_qkv, grad_proj, grad_hidden.astype(jnp.bfloat16), grad_out.astype(jnp.bfloat16))
```

```python
import functools

import jax
import jax.numpy as jnp
from jax import lax
from jax.experimental import pallas as pl
from jax.experimental.pallas import tpu as pltpu
from jax.sharding import Mesh
from jax.sharding import PartitionSpec as P

HEAD_DIM = 64
EPSILON = 1e-05
MESH = pl.DeviceIdType.MESH
BF16 = jnp.bfloat16
F32 = jnp.float32
VMEM = pl.BlockSpec(memory_space=pltpu.VMEM)
SMEM = pl.BlockSpec(memory_space=pltpu.SMEM)
LIMIT = 60 * 1024 * 1024


def dot(a, b, da, db):
    return lax.dot_general(a, b, (((da,), (db,)), ((), ())), preferred_element_type=F32)


def plain(body, outs, ins, scratch=(), flops=1_000_000_000, out_specs=None):
    return pl.pallas_call(
        body,
        out_shape=outs,
        in_specs=ins,
        out_specs=out_specs if out_specs is not None else [VMEM] * len(outs),
        scratch_shapes=scratch,
        compiler_params=pltpu.CompilerParams(vmem_limit_bytes=LIMIT),
        cost_estimate=pl.CostEstimate(flops=flops, bytes_accessed=4_000_000, transcendentals=0),
    )


def place(nx, ny, index, cores):
    if cores == 2:
        chip = index // 2
        return {"x": chip // ny, "y": chip % ny, "c": index % 2}
    return {"x": index // ny, "y": index % ny}


def exchange_body(nx, ny, cores, count, *refs):
    ins, outs, (send, recv, local) = refs[:count], refs[count : 2 * count], refs[2 * count :]
    me = lax.axis_index("x") * ny + lax.axis_index("y")
    if cores == 2:
        me = me * 2 + lax.axis_index("c")
    peers = nx * ny * cores
    barrier = pltpu.get_barrier_semaphore()
    for k in range(1, peers):
        peer = lax.rem(me + k, peers)
        pl.semaphore_signal(barrier, inc=1, device_id=place(nx, ny, peer, cores), device_id_type=MESH)
    own = []
    for a in range(count):
        own.append(pltpu.make_async_copy(ins[a].at[me], outs[a].at[me], local.at[a]))
        own[-1].start()
    pl.semaphore_wait(barrier, peers - 1)
    copies = []
    for a in range(count):
        for k in range(1, peers):
            peer = lax.rem(me + k, peers)
            copies.append(
                pltpu.make_async_remote_copy(
                    src_ref=ins[a].at[peer],
                    dst_ref=outs[a].at[me],
                    send_sem=send.at[a, k],
                    recv_sem=recv.at[a, k],
                    device_id=place(nx, ny, peer, cores),
                    device_id_type=MESH,
                )
            )
            copies[-1].start()
    for copy in own:
        copy.wait()
    for copy in copies:
        copy.wait()


def exchange(arrays, sizes, cores, ident):
    nx, ny = sizes
    peers = nx * ny * cores
    count = len(arrays)
    return pl.pallas_call(
        functools.partial(exchange_body, nx, ny, cores, count),
        out_shape=[jax.ShapeDtypeStruct(a.shape, a.dtype) for a in arrays],
        in_specs=[VMEM] * count,
        out_specs=[VMEM] * count,
        scratch_shapes=[
            pltpu.SemaphoreType.DMA((count, peers)),
            pltpu.SemaphoreType.DMA((count, peers)),
            pltpu.SemaphoreType.DMA((count,)),
        ],
        compiler_params=pltpu.CompilerParams(
            collective_id=ident, has_side_effects=True, vmem_limit_bytes=16 * 1024 * 1024
        ),
        cost_estimate=pl.CostEstimate(flops=1_000_000_000, bytes_accessed=4_000_000, transcendentals=0),
    )(*arrays)


def tiles_body(spec_ref, cot_ref, widths_ref, group_ref, normed_ref, cots_ref, starts_ref, slots_ref, full, counts):
    parts, frames, cols = spec_ref.shape
    groups = counts.shape[0]
    slot_count = normed_ref.shape[0] // groups
    feat = normed_ref.shape[2]
    bands = widths_ref.shape[0]
    for p in range(parts):
        full[0, :, p * cols : (p + 1) * cols] = spec_ref[p].astype(F32)
        full[1, :, p * cols : (p + 1) * cols] = cot_ref[p].astype(F32)
    total = parts * cols
    full[:, :, total:] = jnp.zeros((2, frames, full.shape[2] - total), F32)
    normed_ref[...] = jnp.zeros_like(normed_ref)
    cots_ref[...] = jnp.zeros_like(cots_ref)
    for g in range(groups):
        counts[g] = 0
    window = feat + 128
    lane = lax.broadcasted_iota(jnp.int32, (frames, feat), 1)

    def step(b, start):
        width = widths_ref[b]
        group = group_ref[b]
        rank = counts[group]
        counts[group] = rank + 1
        slot = group * slot_count + rank
        starts_ref[b] = start
        slots_ref[b] = slot
        offset = 4 * start
        base = pl.multiple_of((offset // 128) * 128, 128)
        shift = lax.rem(window - (offset - base), window)
        raw = pltpu.roll(full[0, :, pl.ds(base, window)], shift, 1)[:, :feat]
        cot = pltpu.roll(full[1, :, pl.ds(base, window)], shift, 1)[:, :feat]
        valid = lane < 4 * width
        raw = jnp.where(valid, raw, 0.0)
        cot = jnp.where(valid, cot, 0.0)
        counted = jnp.full((frames, 1), 4 * width, jnp.int32).astype(F32)
        mean = jnp.sum(raw * raw, axis=1, keepdims=True) / counted
        normed_ref[slot] = (raw * lax.rsqrt(mean + EPSILON)).astype(BF16)
        cots_ref[slot] = cot.astype(BF16)
        return start + width

    lax.fori_loop(0, bands, step, jnp.int32(0))


def band_tiles(spec_rows, cot_rows, widths, band_group, groups, slot_count, feat):
    parts, frames, cols = spec_rows.shape
    bands = widths.shape[0]
    tile = jax.ShapeDtypeStruct((groups * slot_count, frames, feat), BF16)
    ints = jax.ShapeDtypeStruct((bands,), jnp.int32)
    return plain(
        tiles_body,
        [tile, tile, ints, ints],
        [VMEM, VMEM, SMEM, SMEM],
        [pltpu.VMEM((2, frames, parts * cols + feat + 128), F32), pltpu.SMEM((groups,), jnp.int32)],
        out_specs=[VMEM, VMEM, SMEM, SMEM],
    )(spec_rows, cot_rows, widths, band_group)


def mask_body(tile_ref, widths_ref, starts_ref, slots_ref, out_ref, full):
    parts, frames, cols = out_ref.shape
    feat = tile_ref.shape[2]
    window = feat + 128
    full[...] = jnp.zeros_like(full)
    lane = lax.broadcasted_iota(jnp.int32, (frames, window), 1)

    def step(b, carry):
        offset = 4 * starts_ref[b]
        base = pl.multiple_of((offset // 128) * 128, 128)
        tile = tile_ref[slots_ref[b]].astype(F32)
        wide = jnp.concatenate([tile, jnp.zeros((frames, 128), F32)], axis=1)
        wide = jnp.where(lane < 4 * widths_ref[b], wide, 0.0)
        full[:, pl.ds(base, window)] += pltpu.roll(wide, offset - base, 1)
        return carry

    lax.fori_loop(0, widths_ref.shape[0], step, 0)
    for p in range(parts):
        out_ref[p] = full[:, p * cols : (p + 1) * cols].astype(BF16)


def mask_rows(tiles, widths, starts, slots, parts, cols):
    frames = tiles.shape[1]
    return plain(
        mask_body,
        [jax.ShapeDtypeStruct((parts, frames, cols), BF16)],
        [VMEM, SMEM, SMEM, SMEM],
        [pltpu.VMEM((frames, parts * cols + tiles.shape[2] + 128), F32)],
    )(tiles, widths, starts, slots)[0]


def embed_body(normed_ref, w_ref, out_ref):
    peers, slots, frames, feat = normed_ref.shape
    for s in range(slots):
        rows = normed_ref[:, s].reshape(peers * frames, feat)
        out_ref[:, s] = dot(rows, w_ref[s], 1, 0).astype(BF16).reshape(peers, frames, -1)


def embed(normed, w):
    peers, slots, frames, _ = normed.shape
    return plain(
        embed_body, [jax.ShapeDtypeStruct((peers, slots, frames, w.shape[2]), BF16)], [VMEM, VMEM]
    )(normed, w)[0]


def embed_grad_body(normed_ref, grad_ref, out_ref):
    peers, slots, frames, feat = normed_ref.shape
    for s in range(slots):
        rows = normed_ref[:, s].reshape(peers * frames, feat)
        grads = grad_ref[:, s].reshape(peers * frames, grad_ref.shape[3])
        out_ref[s] = dot(rows, grads, 0, 0).astype(BF16)


def embed_grad(normed, grads):
    _, slots, _, feat = normed.shape
    return plain(
        embed_grad_body,
        [jax.ShapeDtypeStruct((slots, feat, grads.shape[3]), BF16)],
        [VMEM, VMEM],
    )(normed, grads)[0]


def to_frames(rows, frames, bands):
    out = lax.broadcasted_iota(jnp.int32, (rows, rows), 0)
    src = lax.broadcasted_iota(jnp.int32, (rows, rows), 1)
    return ((out // bands == src % frames) & (out % bands == src // frames)).astype(F32).astype(BF16)


def to_bands(rows, frames, bands):
    out = lax.broadcasted_iota(jnp.int32, (rows, rows), 0)
    src = lax.broadcasted_iota(jnp.int32, (rows, rows), 1)
    return ((src // bands == out % frames) & (src % bands == out // frames)).astype(F32).astype(BF16)


BLOCK = 128


def forward_body(tok_ref, slots_ref, w_qkv_ref, w_proj_ref, mixed_ref, rows_ref, packed_ref, soft_ref, heads_ref, stage):
    _, frames, width = tok_ref.shape
    bands = slots_ref.shape[0]
    rows = bands * frames
    inner = w_proj_ref.shape[0]
    heads = inner // HEAD_DIM
    for b in range(bands):
        stage[b] = tok_ref[slots_ref[b]]
    tokens32 = dot(to_frames(rows, frames, bands), stage[...].reshape(rows, width), 1, 0)
    rows_ref[...] = tokens32.astype(BF16)
    inv = lax.rsqrt(jnp.mean(tokens32 * tokens32, axis=1, keepdims=True) + EPSILON)
    normed = (tokens32 * inv).astype(BF16)
    packed_ref[...] = dot(normed, w_qkv_ref[...], 1, 0).astype(BF16)
    row_id = lax.broadcasted_iota(jnp.int32, (BLOCK, BLOCK), 0) // bands
    col_id = lax.broadcasted_iota(jnp.int32, (BLOCK, BLOCK), 1) // bands
    same = row_id == col_id

    def step(i, carry):
        at = pl.ds(pl.multiple_of(i * BLOCK, BLOCK), BLOCK)
        outs = []
        for h in range(heads):
            lo = h * HEAD_DIM
            q = packed_ref[at, lo : lo + HEAD_DIM]
            k = packed_ref[at, inner + lo : inner + lo + HEAD_DIM]
            v = packed_ref[at, 2 * inner + lo : 2 * inner + lo + HEAD_DIM]
            scores = jnp.where(same, dot(q, k, 1, 1) * HEAD_DIM ** (-0.5), -jnp.inf)
            expd = jnp.exp(scores - jnp.max(scores, axis=1, keepdims=True))
            soft = expd / jnp.sum(expd, axis=1, keepdims=True)
            soft_ref[h, at, :] = soft
            outs.append(dot(soft.astype(BF16), v, 1, 0))
        heads_ref[at, :] = jnp.concatenate(outs, axis=1).astype(BF16)
        return carry

    lax.fori_loop(0, rows // BLOCK, step, 0)
    mixed = (tokens32 + dot(heads_ref[...], w_proj_ref[...], 1, 0)).astype(BF16)
    stage[...] = dot(to_bands(rows, frames, bands), mixed, 1, 0).astype(BF16).reshape(bands, frames, width)
    mixed_ref[...] = jnp.zeros_like(mixed_ref)
    for b in range(bands):
        mixed_ref[slots_ref[b]] = stage[b]


def attention_forward(tokens, slots, w_qkv, w_proj):
    _, frames, width = tokens.shape
    bands = slots.shape[0]
    rows = bands * frames
    inner = w_proj.shape[0]
    return plain(
        forward_body,
        [
            jax.ShapeDtypeStruct(tokens.shape, BF16),
            jax.ShapeDtypeStruct((rows, width), BF16),
            jax.ShapeDtypeStruct((rows, 3 * inner), BF16),
            jax.ShapeDtypeStruct((inner // HEAD_DIM, rows, BLOCK), F32),
            jax.ShapeDtypeStruct((rows, inner), BF16),
        ],
        [VMEM, SMEM, VMEM, VMEM],
        [pltpu.VMEM((bands, frames, width), BF16)],
    )(tokens, slots, w_qkv, w_proj)


def backward_body(
    grad_ref, slots_ref, w_qkv_ref, w_proj_ref, rows_ref, packed_ref, soft_ref, heads_ref,
    out_ref, sums_ref, stage, dheads, dpacked,
):
    _, frames, width = grad_ref.shape
    bands = slots_ref.shape[0]
    rows = bands * frames
    inner = w_proj_ref.shape[0]
    heads = inner // HEAD_DIM
    for b in range(bands):
        stage[b] = grad_ref[slots_ref[b]]
    grad32 = dot(to_frames(rows, frames, bands), stage[...].reshape(rows, width), 1, 0)
    grads = grad32.astype(BF16)
    dheads[...] = dot(grads, w_proj_ref[...], 1, 1).astype(BF16)

    def step(i, carry):
        at = pl.ds(pl.multiple_of(i * BLOCK, BLOCK), BLOCK)
        dq, dk, dv = [], [], []
        for h in range(heads):
            lo = h * HEAD_DIM
            q = packed_ref[at, lo : lo + HEAD_DIM]
            k = packed_ref[at, inner + lo : inner + lo + HEAD_DIM]
            v = packed_ref[at, 2 * inner + lo : 2 * inner + lo + HEAD_DIM]
            g = dheads[at, lo : lo + HEAD_DIM]
            soft = soft_ref[h, at, :]
            p_grad = dot(g, v, 1, 1)
            dv.append(dot(soft.astype(BF16), g, 0, 0))
            spread = soft * (p_grad - jnp.sum(p_grad * soft, axis=1, keepdims=True))
            spread = (spread * HEAD_DIM ** (-0.5)).astype(BF16)
            dq.append(dot(spread, k, 1, 0))
            dk.append(dot(spread, q, 0, 0))
        dpacked[at, :] = jnp.concatenate(dq + dk + dv, axis=1).astype(BF16)
        return carry

    lax.fori_loop(0, rows // BLOCK, step, 0)
    tokens32 = rows_ref[...].astype(F32)
    inv = lax.rsqrt(jnp.mean(tokens32 * tokens32, axis=1, keepdims=True) + EPSILON)
    normed32 = tokens32 * inv
    gn = dot(dpacked[...], w_qkv_ref[...], 1, 1)
    back = grad32 + inv * (gn - normed32 * jnp.mean(gn * normed32, axis=1, keepdims=True))
    stage[...] = (
        dot(to_bands(rows, frames, bands), back.astype(BF16), 1, 0).astype(BF16).reshape(bands, frames, width)
    )
    out_ref[...] = jnp.zeros_like(out_ref)
    for b in range(bands):
        out_ref[slots_ref[b]] = stage[b]
    pieces, depth, _ = sums_ref.shape
    small = inner // pieces
    tall = depth - small
    across = 3 * inner // width
    proj = dot(heads_ref[...], grads, 0, 0).astype(BF16)
    sums_ref[:, tall:, :] = proj.reshape(pieces, small, width)
    normed = normed32.astype(BF16)
    for j in range(across):
        part = dot(normed, dpacked[:, j * width : (j + 1) * width], 0, 0).astype(BF16)
        for i in range(pieces // across):
            sums_ref[i * across + j, :tall, :] = part[i * tall : (i + 1) * tall, :]


def attention_backward(grads, slots, w_qkv, w_proj, saved, pieces):
    _, frames, width = grads.shape
    bands = slots.shape[0]
    rows = bands * frames
    inner = w_proj.shape[0]
    depth = (3 * inner * width + inner * width) // pieces // width
    return plain(
        backward_body,
        [
            jax.ShapeDtypeStruct(grads.shape, BF16),
            jax.ShapeDtypeStruct((pieces, depth, width), BF16),
        ],
        [VMEM, SMEM] + [VMEM] * 6,
        [
            pltpu.VMEM((bands, frames, width), BF16),
            pltpu.VMEM((rows, inner), BF16),
            pltpu.VMEM((rows, 3 * inner), BF16),
        ],
    )(grads, slots, w_qkv, w_proj, *saved)


def unpack_body(sums_ref, qkv_ref, proj_ref):
    pieces, depth, width = sums_ref.shape
    small = proj_ref.shape[0] // pieces
    tall = depth - small
    across = qkv_ref.shape[1] // width
    proj_ref[...] = sums_ref[:, tall:, :].astype(F32).reshape(proj_ref.shape)
    for i in range(pieces // across):
        for j in range(across):
            qkv_ref[i * tall : (i + 1) * tall, j * width : (j + 1) * width] = sums_ref[
                i * across + j, :tall, :
            ].astype(F32)


def tail_body(mixed_ref, cot_ref, wh_ref, wo_ref, mask_ref, dmix_ref, gh_ref, go_ref, normed, hidden, dout, dpre):
    peers, _, frames, width = mixed_ref.shape
    feat = cot_ref.shape[3]
    rows = peers * frames
    chunk = min(rows, 256)
    lump = chunk // frames

    def step(i, carry):
        at = pl.ds(pl.multiple_of(i * chunk, chunk), chunk)
        who = pl.ds(i * lump, lump)
        x = mixed_ref[who, 0].reshape(chunk, width).astype(F32)
        inv = lax.rsqrt(jnp.mean(x * x, axis=1, keepdims=True) + EPSILON)
        n = x * inv
        nb = n.astype(BF16)
        normed[at, :] = nb
        t = jnp.tanh(dot(nb, wh_ref[0], 1, 0))
        hb = t.astype(BF16)
        hidden[at, :] = hb
        out = dot(hb, wo_ref[0], 1, 0)
        value = out[:, :feat]
        gate = jax.nn.sigmoid(out[:, feat:])
        mask_ref[who, 0] = (value * gate).astype(BF16).reshape(lump, frames, feat)
        c = cot_ref[who, 0].reshape(chunk, feat).astype(F32)
        cg = c * gate
        g = jnp.concatenate([cg, cg * value * (1.0 - gate)], axis=1).astype(BF16)
        dout[at, :] = g
        gp = (dot(g, wo_ref[0], 1, 1) * (1.0 - t * t)).astype(BF16)
        dpre[at, :] = gp
        gn = dot(gp, wh_ref[0], 1, 1)
        dm = inv * (gn - n * jnp.mean(gn * n, axis=1, keepdims=True))
        dmix_ref[who, 0] = dm.astype(BF16).reshape(lump, frames, width)
        return carry

    lax.fori_loop(0, rows // chunk, step, 0)
    go_ref[0] = dot(hidden[...], dout[...], 0, 0).astype(BF16)
    gh_ref[0] = dot(normed[...], dpre[...], 0, 0).astype(BF16)


def tail(mixed, cots, w_hidden, w_out):
    peers, slots, frames, width = mixed.shape
    feat = cots.shape[3]
    hid = w_hidden.shape[2]
    rows = peers * frames

    def tile(last):
        return pl.BlockSpec((peers, 1, frames, last), lambda s: (0, s, 0, 0))

    def weight(a, b):
        return pl.BlockSpec((1, a, b), lambda s: (s, 0, 0))

    return pl.pallas_call(
        tail_body,
        grid=(slots,),
        out_shape=[
            jax.ShapeDtypeStruct((peers, slots, frames, feat), BF16),
            jax.ShapeDtypeStruct((peers, slots, frames, width), BF16),
            jax.ShapeDtypeStruct((slots, width, hid), BF16),
            jax.ShapeDtypeStruct((slots, hid, 2 * feat), BF16),
        ],
        in_specs=[tile(width), tile(feat), weight(width, hid), weight(hid, 2 * feat)],
        out_specs=[tile(feat), tile(width), weight(width, hid), weight(hid, 2 * feat)],
        scratch_shapes=[
            pltpu.VMEM((rows, width), BF16),
            pltpu.VMEM((rows, hid), BF16),
            pltpu.VMEM((rows, 2 * feat), BF16),
            pltpu.VMEM((rows, hid), BF16),
        ],
        compiler_params=pltpu.CompilerParams(vmem_limit_bytes=LIMIT),
        cost_estimate=pl.CostEstimate(flops=11_000_000_000, bytes_accessed=12_000_000, transcendentals=0),
    )(mixed, cots, w_hidden, w_out)


def totals_body(nx, ny, nz, x_ref, o_ref, pair, part, landed, mine, deep, final, s_sem, r_sem, s2, r2, s3, r3, s4, r4, s5, r5):
    xi, yi, zi, ci = (lax.axis_index(n) for n in ("x", "y", "z", "c"))
    me = xi * ny + yi
    chips = nx * ny
    other = {"c": 1 - ci}
    barrier = pltpu.get_barrier_semaphore()
    pl.semaphore_signal(barrier, inc=1, device_id=other, device_id_type=MESH)
    for k in range(1, chips):
        pl.semaphore_signal(
            barrier, inc=1, device_id=place(nx, ny, lax.rem(me + k, chips), 1), device_id_type=MESH
        )
    for k in range(1, nz):
        pl.semaphore_signal(barrier, inc=1, device_id={"z": lax.rem(zi + k, nz)}, device_id_type=MESH)
    pl.semaphore_wait(barrier, 1 + chips - 1 + nz - 1)

    def remote(src, dst, send, recv, where):
        return pltpu.make_async_remote_copy(
            src_ref=src, dst_ref=dst, send_sem=send, recv_sem=recv, device_id=where, device_id_type=MESH
        )

    first = [
        remote(x_ref.at[(1 - ci) * chips + lax.rem(me + k, chips)], pair.at[lax.rem(me + k, chips)], s_sem.at[k], r_sem.at[k], other)
        for k in range(chips)
    ]
    for k in list(range(1, chips)) + [0]:
        first[k].start()
    spread = []
    for k in list(range(1, chips)) + [0]:
        first[k].wait()
        q = lax.rem(me + k, chips)
        summed = x_ref[ci * chips + q].astype(F32) + pair[q].astype(F32)
        if k:
            part[q] = summed.astype(BF16)
            spread.append(remote(part.at[q], landed.at[me], s2.at[k], r2.at[k], place(nx, ny, q, 1)))
            spread[-1].start()
        else:
            landed[me] = summed.astype(BF16)
    for copy in spread:
        copy.wait()
    total = landed[0].astype(F32)
    for q in range(1, chips):
        total += landed[q].astype(F32)
    mine[...] = total.astype(BF16)
    deep[zi] = total.astype(BF16)
    across = [
        remote(mine, deep.at[zi], s3.at[k], r3.at[k], {"z": lax.rem(zi + k, nz)}) for k in range(1, nz)
    ]
    for copy in across:
        copy.start()
    for copy in across:
        copy.wait()
    total = deep[0].astype(F32)
    for q in range(1, nz):
        total += deep[q].astype(F32)
    final[...] = total.astype(BF16)
    o_ref[ci * chips + me] = total.astype(BF16)
    back = [
        remote(final, o_ref.at[ci * chips + me], s4.at[k], r4.at[k], place(nx, ny, lax.rem(me + k, chips), 1))
        for k in range(1, chips)
    ]
    for copy in back:
        copy.start()
    shared = [remote(final, o_ref.at[ci * chips + me], s5.at[0], r5.at[0], other)]
    shared[0].start()
    for k in range(1, chips):
        back[k - 1].wait()
        q = ci * chips + lax.rem(me - k + chips, chips)
        shared.append(remote(o_ref.at[q], o_ref.at[q], s5.at[k], r5.at[k], other))
        shared[-1].start()
    for copy in shared:
        copy.wait()


def totals(packed, sizes, nz, ident):
    nx, ny = sizes
    pieces, depth, width = packed.shape
    chips = nx * ny
    dma = pltpu.SemaphoreType.DMA
    block = pltpu.VMEM((depth, width), BF16)
    return pl.pallas_call(
        functools.partial(totals_body, nx, ny, nz),
        out_shape=jax.ShapeDtypeStruct(packed.shape, BF16),
        in_specs=[VMEM],
        out_specs=VMEM,
        scratch_shapes=[
            pltpu.VMEM((chips, depth, width), BF16),
            pltpu.VMEM((chips, depth, width), BF16),
            pltpu.VMEM((chips, depth, width), BF16),
            block,
            pltpu.VMEM((nz, depth, width), BF16),
            block,
            dma((chips,)), dma((chips,)), dma((chips,)), dma((chips,)),
            dma((nz,)), dma((nz,)), dma((chips,)), dma((chips,)), dma((chips,)), dma((chips,)),
        ],
        compiler_params=pltpu.CompilerParams(
            collective_id=ident, has_side_effects=True, vmem_limit_bytes=16 * 1024 * 1024
        ),
        cost_estimate=pl.CostEstimate(flops=1_000_000_000, bytes_accessed=4_000_000, transcendentals=0),
    )(packed)


def summed_over_z(grads, nz):
    slots, rows, cols = grads.shape
    part = rows // nz
    z = lax.axis_index("z")
    down = [(i, (i - 1) % nz) for i in range(nz)]
    up = [(i, (i + 1) % nz) for i in range(nz)]

    def piece(offset, half):
        at = lax.rem(z + offset + nz, nz) * part
        return lax.dynamic_slice(grads, (half * (slots // 2), at, 0), (slots // 2, part, cols))

    one_down = lax.ppermute(piece(2, 0), "z", down)
    one_up = lax.ppermute(piece(2, 1), "z", up)
    side_down = lax.ppermute(piece(nz - 1, 1), "z", down)
    side_up = lax.ppermute(piece(1, 0), "z", up)
    two_down = lax.ppermute((one_down.astype(F32) + piece(nz - 1, 0).astype(F32)).astype(BF16), "z", down)
    two_up = lax.ppermute((one_up.astype(F32) + piece(1, 1).astype(F32)).astype(BF16), "z", up)
    low = piece(0, 0).astype(F32) + two_down.astype(F32) + side_up.astype(F32)
    high = piece(0, 1).astype(F32) + two_up.astype(F32) + side_down.astype(F32)
    return jnp.concatenate([low, high], axis=0).astype(BF16)


def both_cores(part):
    rows = part.shape[1]
    c = lax.axis_index("c")
    half = rows // 2
    kept = lax.dynamic_slice_in_dim(part, c * half, half, 1)
    sent = lax.dynamic_slice_in_dim(part, (1 - c) * half, half, 1)
    other = lax.ppermute(sent, "c", [(0, 1), (1, 0)])
    low = jnp.where(c == 0, kept, other)
    high = jnp.where(c == 0, other, kept)
    return jnp.concatenate([low, high], axis=0).transpose(1, 0, 2)


def per_device(spec, cotangent, widths, band_group, w_embed, w_qkv, w_proj, w_hidden, w_out):
    frames, cols = spec.shape
    feat, slot_count, width = w_embed.shape
    nx, ny, nz = (lax.axis_size(n) for n in ("x", "y", "z"))
    sizes = (nx, ny)
    groups = nx * ny
    peers = groups * 2
    pair = slot_count // 2
    each = frames // groups
    c = lax.axis_index("c")

    def own(w):
        return lax.dynamic_slice_in_dim(w, c * pair, pair, 1).transpose(1, 0, 2)

    we, wh, wo = own(w_embed), own(w_hidden), own(w_out)

    spec_rows, cot_rows = exchange(
        [spec.reshape(groups, each, cols), cotangent.reshape(groups, each, cols)], sizes, 1, 0
    )
    normed, cots, starts, slots = band_tiles(spec_rows, cot_rows, widths, band_group, groups, slot_count, feat)
    four = lambda a: a.reshape(peers, pair, *a.shape[1:])
    flat = lambda a: a.reshape(peers * pair, *a.shape[2:])
    normed, cots = exchange([four(normed), four(cots)], sizes, 2, 1)
    embedded = embed(normed, we)
    (tokens,) = exchange([embedded], sizes, 2, 2)
    mixed, *saved = attention_forward(flat(tokens), slots, w_qkv, w_proj)
    (mixed,) = exchange([four(mixed)], sizes, 2, 3)
    mask_tiles, dmix, grad_hidden, grad_out = tail(mixed, cots, wh, wo)
    grad_out = summed_over_z(grad_out, nz)
    grad_hidden = summed_over_z(grad_hidden, nz)
    dmix, mask_tiles = exchange([dmix, mask_tiles], sizes, 2, 4)
    dtok, sums = attention_backward(flat(dmix), slots, w_qkv, w_proj, saved, peers)
    mask = mask_rows(flat(mask_tiles), widths, starts, slots, groups, cols)
    (dtok,) = exchange([four(dtok)], sizes, 2, 5)
    (mask,) = exchange([mask], sizes, 1, 6)
    grad_embed = summed_over_z(embed_grad(normed, dtok), nz)
    sums = totals(sums, sizes, nz, 7)
    grad_qkv, grad_proj = plain(
        unpack_body,
        [jax.ShapeDtypeStruct(w_qkv.shape, F32), jax.ShapeDtypeStruct(w_proj.shape, F32)],
        [VMEM],
    )(sums)
    return (
        mask.reshape(frames, cols),
        both_cores(grad_embed),
        grad_qkv,
        grad_proj,
        both_cores(grad_hidden),
        both_cores(grad_out),
    )


def solution(mesh):
    split = Mesh(mesh.devices.reshape(4, 4, 4, 2), ("x", "y", "z", "c"))
    band = ("x", "y")
    tm = ("z", "c")
    placed = (
        P(tm, band),
        P(tm, band),
        P(),
        P(),
        P(None, band, None),
        P(),
        P(),
        P(None, band, None),
        P(None, band, None),
    )
    return jax.shard_map(
        per_device,
        mesh=split,
        in_specs=placed,
        out_specs=(
            P(tm, band),
            P(tm, band, None),
            P(),
            P(),
            P(tm, band, None),
            P(tm, band, None),
        ),
        check_vma=False,
    )
```

```python
import functools

import jax
import jax.numpy as jnp
from jax import lax
from jax.experimental import pallas as pl
from jax.experimental.pallas import tpu as pltpu
from jax.sharding import Mesh
from jax.sharding import PartitionSpec as P

HEAD_DIM = 64
EPSILON = 1e-05
MESH = pl.DeviceIdType.MESH
BF16 = jnp.bfloat16
F32 = jnp.float32
VMEM = pl.BlockSpec(memory_space=pltpu.VMEM)
SMEM = pl.BlockSpec(memory_space=pltpu.SMEM)
MIB = 1024 * 1024


def dot(a, b, da, db):
    return lax.dot_general(a, b, (((da,), (db,)), ((), ())), preferred_element_type=F32)


def plain(body, outs, ins, scratch=(), mib=8, out_specs=None):
    return pl.pallas_call(
        body,
        out_shape=outs,
        in_specs=ins,
        out_specs=out_specs if out_specs is not None else [VMEM] * len(outs),
        scratch_shapes=scratch,
        compiler_params=pltpu.CompilerParams(vmem_limit_bytes=mib * MIB),
    )


def place(nx, ny, index, cores):
    if cores == 2:
        chip = index // 2
        return {"x": chip // ny, "y": chip % ny, "c": index % 2}
    return {"x": index // ny, "y": index % ny}


def exchange_body(nx, ny, cores, count, *refs):
    ins, outs, (send, recv, local) = refs[:count], refs[count : 2 * count], refs[2 * count :]
    me = lax.axis_index("x") * ny + lax.axis_index("y")
    if cores == 2:
        me = me * 2 + lax.axis_index("c")
    peers = nx * ny * cores
    barrier = pltpu.get_barrier_semaphore()
    for k in range(1, peers):
        peer = lax.rem(me + k, peers)
        pl.semaphore_signal(barrier, inc=1, device_id=place(nx, ny, peer, cores), device_id_type=MESH)
    own = []
    for a in range(count):
        own.append(pltpu.make_async_copy(ins[a].at[me], outs[a].at[me], local.at[a]))
        own[-1].start()
    pl.semaphore_wait(barrier, peers - 1)
    copies = []
    for a in range(count):
        for k in range(1, peers):
            peer = lax.rem(me + k, peers)
            copies.append(
                pltpu.make_async_remote_copy(
                    src_ref=ins[a].at[peer],
                    dst_ref=outs[a].at[me],
                    send_sem=send.at[a, k],
                    recv_sem=recv.at[a, k],
                    device_id=place(nx, ny, peer, cores),
                    device_id_type=MESH,
                )
            )
            copies[-1].start()
    for copy in own:
        copy.wait()
    for copy in copies:
        copy.wait()


def exchange(arrays, sizes, cores, ident):
    nx, ny = sizes
    peers = nx * ny * cores
    count = len(arrays)
    return pl.pallas_call(
        functools.partial(exchange_body, nx, ny, cores, count),
        out_shape=[jax.ShapeDtypeStruct(a.shape, a.dtype) for a in arrays],
        in_specs=[VMEM] * count,
        out_specs=[VMEM] * count,
        scratch_shapes=[
            pltpu.SemaphoreType.DMA((count, peers)),
            pltpu.SemaphoreType.DMA((count, peers)),
            pltpu.SemaphoreType.DMA((count,)),
        ],
        compiler_params=pltpu.CompilerParams(
            collective_id=ident, has_side_effects=True, vmem_limit_bytes=16 * 1024 * 1024
        ),
    )(*arrays)


def tiles_body(spec_ref, cot_ref, widths_ref, group_ref, normed_ref, cots_ref, starts_ref, slots_ref, full, counts):
    parts, frames, cols = spec_ref.shape
    groups = counts.shape[0]
    slot_count = normed_ref.shape[0] // groups
    feat = normed_ref.shape[2]
    bands = widths_ref.shape[0]
    for p in range(parts):
        full[0, :, p * cols : (p + 1) * cols] = spec_ref[p].astype(F32)
        full[1, :, p * cols : (p + 1) * cols] = cot_ref[p].astype(F32)
    total = parts * cols
    full[:, :, total:] = jnp.zeros((2, frames, full.shape[2] - total), F32)
    normed_ref[...] = jnp.zeros_like(normed_ref)
    cots_ref[...] = jnp.zeros_like(cots_ref)
    for g in range(groups):
        counts[g] = 0
    window = feat + 128
    lane = lax.broadcasted_iota(jnp.int32, (frames, feat), 1)

    def index(b, start):
        group = group_ref[b]
        rank = counts[group]
        counts[group] = rank + 1
        starts_ref[b] = start
        slots_ref[b] = group * slot_count + rank
        return start + widths_ref[b]

    lax.fori_loop(0, bands, index, jnp.int32(0))

    def step(b, carry):
        width = widths_ref[b]
        slot = slots_ref[b]
        start = starts_ref[b]
        offset = 4 * start
        base = pl.multiple_of((offset // 128) * 128, 128)
        shift = lax.rem(window - (offset - base), window)
        raw = pltpu.roll(full[0, :, pl.ds(base, window)], shift, 1)[:, :feat]
        cot = pltpu.roll(full[1, :, pl.ds(base, window)], shift, 1)[:, :feat]
        valid = lane < 4 * width
        raw = jnp.where(valid, raw, 0.0)
        cot = jnp.where(valid, cot, 0.0)
        counted = jnp.full((frames, 1), 4 * width, jnp.int32).astype(F32)
        mean = jnp.sum(raw * raw, axis=1, keepdims=True) / counted
        normed_ref[slot] = (raw * lax.rsqrt(mean + EPSILON)).astype(BF16)
        cots_ref[slot] = cot.astype(BF16)
        return carry

    lax.fori_loop(0, bands, step, 0, unroll=4)


def band_tiles(spec_rows, cot_rows, widths, band_group, groups, slot_count, feat):
    parts, frames, cols = spec_rows.shape
    bands = widths.shape[0]
    tile = jax.ShapeDtypeStruct((groups * slot_count, frames, feat), BF16)
    ints = jax.ShapeDtypeStruct((bands,), jnp.int32)
    return plain(
        tiles_body,
        [tile, tile, ints, ints],
        [VMEM, VMEM, SMEM, SMEM],
        [pltpu.VMEM((2, frames, parts * cols + feat + 128), F32), pltpu.SMEM((groups,), jnp.int32)],
        out_specs=[VMEM, VMEM, SMEM, SMEM],
    )(spec_rows, cot_rows, widths, band_group)


def mask_body(tile_ref, widths_ref, starts_ref, slots_ref, out_ref, full):
    parts, frames, cols = out_ref.shape
    feat = tile_ref.shape[2]
    window = feat + 128
    full[...] = jnp.zeros_like(full)
    lane = lax.broadcasted_iota(jnp.int32, (frames, window), 1)

    def step(b, carry):
        offset = 4 * starts_ref[b]
        base = pl.multiple_of((offset // 128) * 128, 128)
        tile = tile_ref[slots_ref[b]].astype(F32)
        wide = jnp.concatenate([tile, jnp.zeros((frames, 128), F32)], axis=1)
        wide = jnp.where(lane < 4 * widths_ref[b], wide, 0.0)
        full[:, pl.ds(base, window)] += pltpu.roll(wide, offset - base, 1)
        return carry

    lax.fori_loop(0, widths_ref.shape[0], step, 0)
    for p in range(parts):
        out_ref[p] = full[:, p * cols : (p + 1) * cols].astype(BF16)


def mask_rows(tiles, widths, starts, slots, parts, cols):
    frames = tiles.shape[1]
    return plain(
        mask_body,
        [jax.ShapeDtypeStruct((parts, frames, cols), BF16)],
        [VMEM, SMEM, SMEM, SMEM],
        [pltpu.VMEM((frames, parts * cols + tiles.shape[2] + 128), F32)],
    )(tiles, widths, starts, slots)[0]


def embed_body(normed_ref, w_ref, out_ref):
    peers, slots, frames, feat = normed_ref.shape
    for s in range(slots):
        rows = normed_ref[:, s].reshape(peers * frames, feat)
        out_ref[:, s] = dot(rows, w_ref[s], 1, 0).astype(BF16).reshape(peers, frames, -1)


def embed(normed, w):
    peers, slots, frames, _ = normed.shape
    return plain(
        embed_body, [jax.ShapeDtypeStruct((peers, slots, frames, w.shape[2]), BF16)], [VMEM, VMEM]
    )(normed, w)[0]


def embed_grad_body(normed_ref, grad_ref, out_ref):
    peers, slots, frames, feat = normed_ref.shape
    for s in range(slots):
        rows = normed_ref[:, s].reshape(peers * frames, feat)
        grads = grad_ref[:, s].reshape(peers * frames, grad_ref.shape[3])
        out_ref[s] = dot(rows, grads, 0, 0).astype(BF16)


def embed_grad(normed, grads):
    _, slots, _, feat = normed.shape
    return plain(
        embed_grad_body,
        [jax.ShapeDtypeStruct((slots, feat, grads.shape[3]), BF16)],
        [VMEM, VMEM],
    )(normed, grads)[0]


def to_frames(rows, frames, bands):
    out = lax.broadcasted_iota(jnp.int32, (rows, rows), 0)
    src = lax.broadcasted_iota(jnp.int32, (rows, rows), 1)
    return ((out // bands == src % frames) & (out % bands == src // frames)).astype(F32).astype(BF16)


def to_bands(rows, frames, bands):
    out = lax.broadcasted_iota(jnp.int32, (rows, rows), 0)
    src = lax.broadcasted_iota(jnp.int32, (rows, rows), 1)
    return ((src // bands == out % frames) & (src % bands == out // frames)).astype(F32).astype(BF16)


BLOCK = 128


def forward_body(tok_ref, slots_ref, w_qkv_ref, w_proj_ref, mixed_ref, rows_ref, packed_ref, soft_ref, heads_ref, stage):
    _, frames, width = tok_ref.shape
    bands = slots_ref.shape[0]
    rows = bands * frames
    inner = w_proj_ref.shape[0]
    heads = inner // HEAD_DIM
    for b in range(bands):
        stage[b] = tok_ref[slots_ref[b]]
    tokens32 = dot(to_frames(rows, frames, bands), stage[...].reshape(rows, width), 1, 0)
    rows_ref[...] = tokens32.astype(BF16)
    inv = lax.rsqrt(jnp.mean(tokens32 * tokens32, axis=1, keepdims=True) + EPSILON)
    normed = (tokens32 * inv).astype(BF16)
    packed_ref[...] = dot(normed, w_qkv_ref[...], 1, 0).astype(BF16)
    row_id = lax.broadcasted_iota(jnp.int32, (BLOCK, BLOCK), 0) // bands
    col_id = lax.broadcasted_iota(jnp.int32, (BLOCK, BLOCK), 1) // bands
    same = row_id == col_id

    def step(i, carry):
        at = pl.ds(pl.multiple_of(i * BLOCK, BLOCK), BLOCK)
        outs = []
        for h in range(heads):
            lo = h * HEAD_DIM
            q = packed_ref[at, lo : lo + HEAD_DIM]
            k = packed_ref[at, inner + lo : inner + lo + HEAD_DIM]
            v = packed_ref[at, 2 * inner + lo : 2 * inner + lo + HEAD_DIM]
            scores = jnp.where(same, dot(q, k, 1, 1) * HEAD_DIM ** (-0.5), -jnp.inf)
            expd = jnp.exp(scores - jnp.max(scores, axis=1, keepdims=True))
            soft = expd / jnp.sum(expd, axis=1, keepdims=True)
            soft_ref[h, at, :] = soft
            outs.append(dot(soft.astype(BF16), v, 1, 0))
        heads_ref[at, :] = jnp.concatenate(outs, axis=1).astype(BF16)
        return carry

    lax.fori_loop(0, rows // BLOCK, step, 0)
    mixed = (tokens32 + dot(heads_ref[...], w_proj_ref[...], 1, 0)).astype(BF16)
    stage[...] = dot(to_bands(rows, frames, bands), mixed, 1, 0).astype(BF16).reshape(bands, frames, width)
    mixed_ref[...] = jnp.zeros_like(mixed_ref)
    for b in range(bands):
        mixed_ref[slots_ref[b]] = stage[b]


def attention_forward(tokens, slots, w_qkv, w_proj):
    _, frames, width = tokens.shape
    bands = slots.shape[0]
    rows = bands * frames
    inner = w_proj.shape[0]
    return plain(
        forward_body,
        [
            jax.ShapeDtypeStruct(tokens.shape, BF16),
            jax.ShapeDtypeStruct((rows, width), BF16),
            jax.ShapeDtypeStruct((rows, 3 * inner), BF16),
            jax.ShapeDtypeStruct((inner // HEAD_DIM, rows, BLOCK), F32),
            jax.ShapeDtypeStruct((rows, inner), BF16),
        ],
        [VMEM, SMEM, VMEM, VMEM],
        [pltpu.VMEM((bands, frames, width), BF16)],
        mib=14,
    )(tokens, slots, w_qkv, w_proj)


def backward_body(
    grad_ref, slots_ref, w_qkv_ref, w_proj_ref, rows_ref, packed_ref, soft_ref, heads_ref,
    out_ref, sums_ref, stage, dheads, dpacked,
):
    _, frames, width = grad_ref.shape
    bands = slots_ref.shape[0]
    rows = bands * frames
    inner = w_proj_ref.shape[0]
    heads = inner // HEAD_DIM
    for b in range(bands):
        stage[b] = grad_ref[slots_ref[b]]
    grad32 = dot(to_frames(rows, frames, bands), stage[...].reshape(rows, width), 1, 0)
    grads = grad32.astype(BF16)
    dheads[...] = dot(grads, w_proj_ref[...], 1, 1).astype(BF16)

    def step(i, carry):
        at = pl.ds(pl.multiple_of(i * BLOCK, BLOCK), BLOCK)
        dq, dk, dv = [], [], []
        for h in range(heads):
            lo = h * HEAD_DIM
            q = packed_ref[at, lo : lo + HEAD_DIM]
            k = packed_ref[at, inner + lo : inner + lo + HEAD_DIM]
            v = packed_ref[at, 2 * inner + lo : 2 * inner + lo + HEAD_DIM]
            g = dheads[at, lo : lo + HEAD_DIM]
            soft = soft_ref[h, at, :]
            p_grad = dot(g, v, 1, 1)
            dv.append(dot(soft.astype(BF16), g, 0, 0))
            spread = soft * (p_grad - jnp.sum(p_grad * soft, axis=1, keepdims=True))
            spread = (spread * HEAD_DIM ** (-0.5)).astype(BF16)
            dq.append(dot(spread, k, 1, 0))
            dk.append(dot(spread, q, 0, 0))
        dpacked[at, :] = jnp.concatenate(dq + dk + dv, axis=1).astype(BF16)
        return carry

    lax.fori_loop(0, rows // BLOCK, step, 0)
    tokens32 = rows_ref[...].astype(F32)
    inv = lax.rsqrt(jnp.mean(tokens32 * tokens32, axis=1, keepdims=True) + EPSILON)
    normed32 = tokens32 * inv
    gn = dot(dpacked[...], w_qkv_ref[...], 1, 1)
    back = grad32 + inv * (gn - normed32 * jnp.mean(gn * normed32, axis=1, keepdims=True))
    stage[...] = (
        dot(to_bands(rows, frames, bands), back.astype(BF16), 1, 0).astype(BF16).reshape(bands, frames, width)
    )
    out_ref[...] = jnp.zeros_like(out_ref)
    for b in range(bands):
        out_ref[slots_ref[b]] = stage[b]
    pieces, depth, _ = sums_ref.shape
    small = inner // pieces
    tall = depth - small
    across = 3 * inner // width
    proj = dot(heads_ref[...], grads, 0, 0).astype(BF16)
    sums_ref[:, tall:, :] = proj.reshape(pieces, small, width)
    normed = normed32.astype(BF16)
    for j in range(across):
        part = dot(normed, dpacked[:, j * width : (j + 1) * width], 0, 0).astype(BF16)
        for i in range(pieces // across):
            sums_ref[i * across + j, :tall, :] = part[i * tall : (i + 1) * tall, :]


def attention_backward(grads, slots, w_qkv, w_proj, saved, pieces):
    _, frames, width = grads.shape
    bands = slots.shape[0]
    rows = bands * frames
    inner = w_proj.shape[0]
    depth = (3 * inner * width + inner * width) // pieces // width
    return plain(
        backward_body,
        [
            jax.ShapeDtypeStruct(grads.shape, BF16),
            jax.ShapeDtypeStruct((pieces, depth, width), BF16),
        ],
        [VMEM, SMEM] + [VMEM] * 6,
        [
            pltpu.VMEM((bands, frames, width), BF16),
            pltpu.VMEM((rows, inner), BF16),
            pltpu.VMEM((rows, 3 * inner), BF16),
        ],
        mib=20,
    )(grads, slots, w_qkv, w_proj, *saved)


def unpack_body(sums_ref, qkv_ref, proj_ref):
    pieces, depth, width = sums_ref.shape
    small = proj_ref.shape[0] // pieces
    tall = depth - small
    across = qkv_ref.shape[1] // width
    proj_ref[...] = sums_ref[:, tall:, :].astype(F32).reshape(proj_ref.shape)
    for i in range(pieces // across):
        for j in range(across):
            qkv_ref[i * tall : (i + 1) * tall, j * width : (j + 1) * width] = sums_ref[
                i * across + j, :tall, :
            ].astype(F32)


def tail_body(mixed_ref, cot_ref, wh_ref, wo_ref, mask_ref, dmix_ref, gh_ref, go_ref, normed, hidden, dout, dpre):
    peers, _, frames, width = mixed_ref.shape
    feat = cot_ref.shape[3]
    rows = peers * frames
    chunk = min(rows, 256)
    lump = chunk // frames

    def step(i, carry):
        at = pl.ds(pl.multiple_of(i * chunk, chunk), chunk)
        who = pl.ds(i * lump, lump)
        x = mixed_ref[who, 0].reshape(chunk, width).astype(F32)
        inv = lax.rsqrt(jnp.mean(x * x, axis=1, keepdims=True) + EPSILON)
        n = x * inv
        nb = n.astype(BF16)
        normed[at, :] = nb
        t = jnp.tanh(dot(nb, wh_ref[0], 1, 0))
        hb = t.astype(BF16)
        hidden[at, :] = hb
        out = dot(hb, wo_ref[0], 1, 0)
        value = out[:, :feat]
        gate = jax.nn.sigmoid(out[:, feat:])
        mask_ref[who, 0] = (value * gate).astype(BF16).reshape(lump, frames, feat)
        c = cot_ref[who, 0].reshape(chunk, feat).astype(F32)
        cg = c * gate
        g = jnp.concatenate([cg, cg * value * (1.0 - gate)], axis=1).astype(BF16)
        dout[at, :] = g
        gp = (dot(g, wo_ref[0], 1, 1) * (1.0 - t * t)).astype(BF16)
        dpre[at, :] = gp
        gn = dot(gp, wh_ref[0], 1, 1)
        dm = inv * (gn - n * jnp.mean(gn * n, axis=1, keepdims=True))
        dmix_ref[who, 0] = dm.astype(BF16).reshape(lump, frames, width)
        return carry

    lax.fori_loop(0, rows // chunk, step, 0)
    go_ref[0] = dot(hidden[...], dout[...], 0, 0).astype(BF16)
    gh_ref[0] = dot(normed[...], dpre[...], 0, 0).astype(BF16)


def tail(mixed, cots, w_hidden, w_out):
    peers, slots, frames, width = mixed.shape
    feat = cots.shape[3]
    hid = w_hidden.shape[2]
    rows = peers * frames

    def tile(last):
        return pl.BlockSpec((peers, 1, frames, last), lambda s: (0, s, 0, 0))

    def weight(a, b):
        return pl.BlockSpec((1, a, b), lambda s: (s, 0, 0))

    return pl.pallas_call(
        tail_body,
        grid=(slots,),
        out_shape=[
            jax.ShapeDtypeStruct((peers, slots, frames, feat), BF16),
            jax.ShapeDtypeStruct((peers, slots, frames, width), BF16),
            jax.ShapeDtypeStruct((slots, width, hid), BF16),
            jax.ShapeDtypeStruct((slots, hid, 2 * feat), BF16),
        ],
        in_specs=[tile(width), tile(feat), weight(width, hid), weight(hid, 2 * feat)],
        out_specs=[tile(feat), tile(width), weight(width, hid), weight(hid, 2 * feat)],
        scratch_shapes=[
            pltpu.VMEM((rows, width), BF16),
            pltpu.VMEM((rows, hid), BF16),
            pltpu.VMEM((rows, 2 * feat), BF16),
            pltpu.VMEM((rows, hid), BF16),
        ],
        compiler_params=pltpu.CompilerParams(vmem_limit_bytes=24 * MIB),
    )(mixed, cots, w_hidden, w_out)


def remote(src, dst, send, recv, where):
    return pltpu.make_async_remote_copy(
        src_ref=src, dst_ref=dst, send_sem=send, recv_sem=recv, device_id=where, device_id_type=MESH
    )


def rows_of(ref, slot, step, nz):
    part = ref.shape[1] // nz
    at = lax.rem(lax.axis_index("z") + step + nz, nz) * part
    return ref.at[slot, pl.ds(pl.multiple_of(at, part), part)]


def z_place(step, nz):
    return {"z": lax.rem(lax.axis_index("z") + step + nz, nz)}


def far_sends(ref, down, up, send, recv, nz):
    return [
        remote(rows_of(ref, 0, 2, nz), down, send.at[0], recv.at[0], z_place(-1, nz)),
        remote(rows_of(ref, 1, 2, nz), up, send.at[1], recv.at[1], z_place(1, nz)),
    ]


def side_sends(ref, down, up, send, recv, nz):
    return [
        remote(rows_of(ref, 1, -1, nz), down, send.at[0], recv.at[0], z_place(-1, nz)),
        remote(rows_of(ref, 0, 1, nz), up, send.at[1], recv.at[1], z_place(1, nz)),
    ]


def near_sends(down_src, up_src, down, up, send, recv, nz):
    return [
        remote(down_src, down, send.at[0], recv.at[0], z_place(-1, nz)),
        remote(up_src, up, send.at[1], recv.at[1], z_place(1, nz)),
    ]


def add_own(ref, received, out, slot, step, nz):
    out[...] = (received[...].astype(F32) + rows_of(ref, slot, step, nz)[...].astype(F32)).astype(BF16)


def spread_body(nx, ny, nz, *refs):
    (dmix, tiles, go, gh, o_dmix, o_tiles, o_down, o_up, h_down, h_up) = refs[:10]
    (ro_down, ro_up, rh_down, rh_up, send, recv, local, zs, zr) = refs[10:]
    me = (lax.axis_index("x") * ny + lax.axis_index("y")) * 2 + lax.axis_index("c")
    peers = nx * ny * 2
    barrier = pltpu.get_barrier_semaphore()
    for k in range(1, peers):
        pl.semaphore_signal(
            barrier, inc=1, device_id=place(nx, ny, lax.rem(me + k, peers), 2), device_id_type=MESH
        )
    for step in (-1, 1):
        pl.semaphore_signal(barrier, inc=1, device_id=z_place(step, nz), device_id_type=MESH)
    pl.semaphore_wait(barrier, peers - 1 + 2)
    first = far_sends(go, ro_down, ro_up, zs.at[0], zr.at[0], nz)
    second = far_sends(gh, rh_down, rh_up, zs.at[1], zr.at[1], nz)
    copies = []
    for copy in first + second:
        copy.start()
    for a, (src, dst) in enumerate(((dmix, o_dmix), (tiles, o_tiles))):
        for k in range(1, peers):
            peer = lax.rem(me + k, peers)
            copies.append(
                remote(src.at[peer], dst.at[me], send.at[a, k], recv.at[a, k], place(nx, ny, peer, 2))
            )
            copies[-1].start()
    own = [
        pltpu.make_async_copy(dmix.at[me], o_dmix.at[me], local.at[0]),
        pltpu.make_async_copy(tiles.at[me], o_tiles.at[me], local.at[1]),
    ]
    for copy in own:
        copy.start()
    for copy in first + second:
        copy.wait()
    add_own(go, ro_down, o_down, 0, -1, nz)
    add_own(go, ro_up, o_up, 1, 1, nz)
    add_own(gh, rh_down, h_down, 0, -1, nz)
    add_own(gh, rh_up, h_up, 1, 1, nz)
    for copy in own + copies:
        copy.wait()


def spread(dmix, tiles, go, gh, sizes, nz, ident):
    peers = dmix.shape[0]
    shape_o = (go.shape[1] // nz, go.shape[2])
    shape_h = (gh.shape[1] // nz, gh.shape[2])
    dma = pltpu.SemaphoreType.DMA
    out = [jax.ShapeDtypeStruct(a, BF16) for a in (dmix.shape, tiles.shape, shape_o, shape_o, shape_h, shape_h)]
    return pl.pallas_call(
        functools.partial(spread_body, *sizes, nz),
        out_shape=out,
        in_specs=[VMEM] * 4,
        out_specs=[VMEM] * 6,
        scratch_shapes=[pltpu.VMEM(a, BF16) for a in (shape_o, shape_o, shape_h, shape_h)]
        + [dma((2, peers)), dma((2, peers)), dma((2,)), dma((2, 2)), dma((2, 2))],
        compiler_params=pltpu.CompilerParams(
            collective_id=ident, has_side_effects=True, vmem_limit_bytes=8 * 1024 * 1024
        ),
    )(dmix, tiles, go, gh)


def finish_body(nx, ny, nz, *refs):
    (x_ref, dtok, mask, normed, go, gh, so_down, so_up, sh_down, sh_up) = refs[:10]
    (o_ref, e_out, out_o, out_h, mask_out) = refs[10:15]
    (pair, part, landed, mine, deep, final, dgrad, ge, e_one_d, e_one_u, e_src_d, e_src_u) = refs[15:27]
    sides, nears = refs[27:33], refs[33:39]
    swaps = refs[39:42]
    (s1, r1, s2, r2, s3, r3, s4, r4, s5, r5, sd, rd, sm, rm, zs, zr, sw, rw, local) = refs[42:]
    xi, yi, zi, ci = (lax.axis_index(n) for n in ("x", "y", "z", "c"))
    me = xi * ny + yi
    chips = nx * ny
    peers = chips * 2
    who = me * 2 + ci
    other = {"c": 1 - ci}
    barrier = pltpu.get_barrier_semaphore()
    for k in range(1, peers):
        pl.semaphore_signal(
            barrier, inc=1, device_id=place(nx, ny, lax.rem(who + k, peers), 2), device_id_type=MESH
        )
    for k in range(1, nz):
        pl.semaphore_signal(barrier, inc=1, device_id={"z": lax.rem(zi + k, nz)}, device_id_type=MESH)
    pl.semaphore_wait(barrier, peers - 1 + nz - 1)

    first = [
        remote(
            x_ref.at[(1 - ci) * chips + lax.rem(me + k, chips)],
            pair.at[lax.rem(me + k, chips)],
            s1.at[k],
            r1.at[k],
            other,
        )
        for k in range(chips)
    ]
    for k in list(range(1, chips)) + [0]:
        first[k].start()
    near = near_sends(so_down, so_up, nears[0], nears[1], zs.at[0], zr.at[0], nz)
    near += near_sends(sh_down, sh_up, nears[2], nears[3], zs.at[1], zr.at[1], nz)
    near += side_sends(go, sides[0], sides[1], zs.at[2], zr.at[2], nz)
    near += side_sends(gh, sides[2], sides[3], zs.at[3], zr.at[3], nz)
    for copy in near:
        copy.start()
    rest = []
    for k in range(1, chips):
        q = lax.rem(me + k, chips)
        rest.append(remote(mask.at[q], mask_out.at[me], sm.at[k], rm.at[k], place(nx, ny, q, 1)))
        rest[-1].start()
    own = [
        pltpu.make_async_copy(mask.at[me], mask_out.at[me], local.at[0]),
        pltpu.make_async_copy(dtok.at[who], dgrad.at[who], local.at[1]),
    ]
    for copy in own:
        copy.start()
    spread_sums = []
    for k in list(range(1, chips)) + [0]:
        first[k].wait()
        q = lax.rem(me + k, chips)
        summed = (x_ref[ci * chips + q].astype(F32) + pair[q].astype(F32)).astype(BF16)
        if k:
            part[q] = summed
            spread_sums.append(remote(part.at[q], landed.at[me], s2.at[k], r2.at[k], place(nx, ny, q, 1)))
            spread_sums[-1].start()
        else:
            landed[me] = summed
    grads = []
    for k in range(1, peers):
        peer = lax.rem(who + k, peers)
        grads.append(remote(dtok.at[peer], dgrad.at[who], sd.at[k], rd.at[k], place(nx, ny, peer, 2)))
        grads[-1].start()
    for copy in spread_sums:
        copy.wait()
    total = landed[0].astype(F32)
    for q in range(1, chips):
        total += landed[q].astype(F32)
    mine[...] = total.astype(BF16)
    deep[zi] = total.astype(BF16)
    across = [
        remote(mine, deep.at[zi], s3.at[k], r3.at[k], {"z": lax.rem(zi + k, nz)}) for k in range(1, nz)
    ]
    for copy in across:
        copy.start()
    for copy in across:
        copy.wait()
    total = deep[0].astype(F32)
    for q in range(1, nz):
        total += deep[q].astype(F32)
    final[...] = total.astype(BF16)
    o_ref[ci * chips + me] = total.astype(BF16)
    back = []
    for k in range(1, chips):
        back.append(
            remote(final, o_ref.at[ci * chips + me], s4.at[k], r4.at[k], place(nx, ny, lax.rem(me + k, chips), 1))
        )
        back[-1].start()
    shared = [remote(final, o_ref.at[ci * chips + me], s5.at[0], r5.at[0], other)]
    shared[0].start()

    def split(grad, near_d, near_u, side_d, side_u, out, swap, job):
        half = out.shape[2]
        for slot, (a, b) in enumerate(((near_d, side_u), (near_u, side_d))):
            own_rows = rows_of(grad, slot, 0, nz)[...].astype(F32)
            rows = (own_rows + a[...].astype(F32) + b[...].astype(F32)).astype(BF16)
            low, high = rows[:half], rows[half:]
            out[ci, slot] = jnp.where(ci == 0, low, high)
            swap[slot] = jnp.where(ci == 0, high, low)
        rest.append(remote(swap, out.at[ci], sw.at[job], rw.at[job], other))
        rest[-1].start()

    for copy in own + grads:
        copy.wait()
    _, slots, frames, feat = normed.shape
    for s in range(slots):
        left = normed[:, s].reshape(peers * frames, feat)
        right = dgrad[:, s].reshape(peers * frames, dgrad.shape[3])
        ge[s] = dot(left, right, 0, 0).astype(BF16)
    e_far = far_sends(ge, e_one_d, e_one_u, zs.at[4], zr.at[4], nz)
    e_side = side_sends(ge, sides[4], sides[5], zs.at[5], zr.at[5], nz)
    for copy in e_far + e_side:
        copy.start()
    for copy in near:
        copy.wait()
    split(go, nears[0], nears[1], sides[0], sides[1], out_o, swaps[0], 0)
    split(gh, nears[2], nears[3], sides[2], sides[3], out_h, swaps[1], 1)
    for copy in e_far:
        copy.wait()
    add_own(ge, e_one_d, e_src_d, 0, -1, nz)
    add_own(ge, e_one_u, e_src_u, 1, 1, nz)
    e_near = near_sends(e_src_d, e_src_u, nears[4], nears[5], zs.at[6], zr.at[6], nz)
    for copy in e_near:
        copy.start()
    for copy in e_side + e_near:
        copy.wait()
    split(ge, nears[4], nears[5], sides[4], sides[5], e_out, swaps[2], 2)
    for k in range(1, chips):
        back[k - 1].wait()
        q = ci * chips + lax.rem(me - k + chips, chips)
        shared.append(remote(o_ref.at[q], o_ref.at[q], s5.at[k], r5.at[k], other))
        shared[-1].start()
    for copy in rest + shared:
        copy.wait()


def finish(packed, dtok, mask, normed, go, gh, srcs, sizes, nz, ident):
    nx, ny = sizes
    pieces, depth, width = packed.shape
    chips = nx * ny
    peers = dtok.shape[0]
    slots, feat = normed.shape[1], normed.shape[3]
    dma = pltpu.SemaphoreType.DMA

    def vmem(*shape):
        return pltpu.VMEM(shape, BF16)

    def parts(rows, cols):
        return vmem(rows // nz, cols)

    dims = [(go.shape[1], go.shape[2]), (gh.shape[1], gh.shape[2]), (feat, width)]
    halves = [(slots, r // nz // 2, c) for r, c in dims]
    block = vmem(depth, width)
    each = [parts(*d) for d in dims for _ in range(2)]
    scratch = [
        vmem(chips, depth, width), vmem(chips, depth, width), vmem(chips, depth, width),
        block, vmem(nz, depth, width), block,
        vmem(*dtok.shape), vmem(slots, feat, width),
    ]
    scratch += [parts(feat, width) for _ in range(4)]
    scratch += each + each + [vmem(*h) for h in halves]
    scratch += [dma((chips,)) for _ in range(4)] + [dma((nz,)) for _ in range(2)] + [dma((chips,)) for _ in range(4)]
    scratch += [dma((peers,)), dma((peers,)), dma((chips,)), dma((chips,))]
    scratch += [dma((7, 2)), dma((7, 2)), dma((3,)), dma((3,)), dma((2,))]
    outs = [packed.shape, (2, *halves[2]), (2, *halves[0]), (2, *halves[1]), mask.shape]
    return pl.pallas_call(
        functools.partial(finish_body, nx, ny, nz),
        out_shape=[jax.ShapeDtypeStruct(o, BF16) for o in outs],
        in_specs=[VMEM] * 10,
        out_specs=[VMEM] * 5,
        scratch_shapes=scratch,
        compiler_params=pltpu.CompilerParams(
            collective_id=ident, has_side_effects=True, vmem_limit_bytes=20 * 1024 * 1024
        ),
    )(packed, dtok, mask, normed, go, gh, *srcs)


def interleaved(halves):
    return halves.reshape(-1, *halves.shape[2:]).transpose(1, 0, 2)


def per_device(spec, cotangent, widths, band_group, w_embed, w_qkv, w_proj, w_hidden, w_out):
    frames, cols = spec.shape
    feat, slot_count, width = w_embed.shape
    nx, ny, nz = (lax.axis_size(n) for n in ("x", "y", "z"))
    sizes = (nx, ny)
    groups = nx * ny
    peers = groups * 2
    pair = slot_count // 2
    each = frames // groups
    c = lax.axis_index("c")

    def own(w):
        return lax.dynamic_slice_in_dim(w, c * pair, pair, 1).transpose(1, 0, 2)

    we, wh, wo = own(w_embed), own(w_hidden), own(w_out)

    spec_rows, cot_rows = exchange(
        [spec.reshape(groups, each, cols), cotangent.reshape(groups, each, cols)], sizes, 1, 0
    )
    normed, cots, starts, slots = band_tiles(spec_rows, cot_rows, widths, band_group, groups, slot_count, feat)
    four = lambda a: a.reshape(peers, pair, *a.shape[1:])
    flat = lambda a: a.reshape(peers * pair, *a.shape[2:])
    normed, cots = exchange([four(normed), four(cots)], sizes, 2, 1)
    embedded = embed(normed, we)
    (tokens,) = exchange([embedded], sizes, 2, 2)
    mixed, *saved = attention_forward(flat(tokens), slots, w_qkv, w_proj)
    (mixed,) = exchange([four(mixed)], sizes, 2, 3)
    mask_tiles, dmix, grad_hidden, grad_out = tail(mixed, cots, wh, wo)
    dmix, mask_tiles, *srcs = spread(dmix, mask_tiles, grad_out, grad_hidden, sizes, nz, 4)
    dtok, sums = attention_backward(flat(dmix), slots, w_qkv, w_proj, saved, peers)
    mask = mask_rows(flat(mask_tiles), widths, starts, slots, groups, cols)
    sums, grad_embed, grad_out, grad_hidden, mask = finish(
        sums, four(dtok), mask, normed, grad_out, grad_hidden, srcs, sizes, nz, 5
    )
    grad_qkv, grad_proj = plain(
        unpack_body,
        [jax.ShapeDtypeStruct(w_qkv.shape, F32), jax.ShapeDtypeStruct(w_proj.shape, F32)],
        [VMEM],
    )(sums)
    return (
        mask.reshape(frames, cols),
        interleaved(grad_embed),
        grad_qkv,
        grad_proj,
        interleaved(grad_hidden),
        interleaved(grad_out),
    )


def solution(mesh):
    split = Mesh(mesh.devices.reshape(4, 4, 4, 2), ("x", "y", "z", "c"))
    band = ("x", "y")
    tm = ("z", "c")
    placed = (
        P(tm, band),
        P(tm, band),
        P(),
        P(),
        P(None, band, None),
        P(),
        P(),
        P(None, band, None),
        P(None, band, None),
    )
    return jax.shard_map(
        per_device,
        mesh=split,
        in_specs=placed,
        out_specs=(
            P(tm, band),
            P(tm, band, None),
            P(),
            P(),
            P(tm, band, None),
            P(tm, band, None),
        ),
        check_vma=False,
    )
```

```python
import functools

import jax
import jax.numpy as jnp
from jax import lax
from jax.experimental import pallas as pl
from jax.experimental.pallas import tpu as pltpu
from jax.sharding import Mesh
from jax.sharding import PartitionSpec as P

HEAD_DIM = 64
EPSILON = 1e-05
MESH = pl.DeviceIdType.MESH
BF16 = jnp.bfloat16
F32 = jnp.float32
VMEM = pl.BlockSpec(memory_space=pltpu.VMEM)
SMEM = pl.BlockSpec(memory_space=pltpu.SMEM)
ANY = pl.BlockSpec(memory_space=pl.ANY)
MIB = 1024 * 1024
BLOCK = 128
FAR_AWAY = 1 << 20


def dot(a, b, da, db):
    return lax.dot_general(a, b, (((da,), (db,)), ((), ())), preferred_element_type=F32)


TABLE = 64
SLOT, START, COLUMNS, OFFSET, SLOT_BAND, SLOT_COLUMNS, SLOT_BASE, SLOT_OFFSET, PICK = (TABLE * i for i in range(9))


def tables_body(groups, slot_count, blocks, widths_ref, group_ref, out_ref, counts):
    bands = widths_ref.shape[0]

    def clear(j, carry):
        out_ref[START + j] = FAR_AWAY
        for row in (SLOT, COLUMNS, OFFSET, SLOT_BAND, SLOT_COLUMNS, SLOT_BASE, SLOT_OFFSET):
            out_ref[row + j] = 0
        return carry

    lax.fori_loop(0, TABLE, clear, 0)
    for g in range(groups):
        counts[g] = 0

    def index(b, start):
        group = group_ref[b]
        width = widths_ref[b]
        rank = counts[group]
        counts[group] = rank + 1
        slot = group * slot_count + rank
        out_ref[SLOT + b] = slot
        out_ref[START + b] = start
        out_ref[COLUMNS + b] = 4 * width
        out_ref[OFFSET + b] = 4 * (start % 32)
        out_ref[SLOT_BAND + slot] = b
        out_ref[SLOT_COLUMNS + slot] = 4 * width
        out_ref[SLOT_BASE + slot] = start // 32
        out_ref[SLOT_OFFSET + slot] = 4 * (start % 32)
        return start + width

    lax.fori_loop(0, bands, index, jnp.int32(0))

    def locate(i, b):
        for _ in range(2):
            b = b + jnp.where(out_ref[START + b + 1] <= 32 * i, 1, 0)
        for r in range(3):
            start = out_ref[START + b + r]
            inside = (start < 32 * i + 32) & (i - start // 32 < 3)
            out_ref[PICK + 3 * i + r] = jnp.where(inside, 3 * (b + r) + i - start // 32, 3 * bands)
        return b

    lax.fori_loop(0, blocks, locate, jnp.int32(0))


def tables(widths, band_group, groups, slot_count, blocks):
    return pl.pallas_call(
        functools.partial(tables_body, groups, slot_count, blocks),
        out_shape=jax.ShapeDtypeStruct((8 * TABLE + 128,), jnp.int32),
        in_specs=[SMEM, SMEM],
        out_specs=SMEM,
        scratch_shapes=[pltpu.SMEM((groups,), jnp.int32)],
    )(widths, band_group)


def remote(src, dst, send, recv, where):
    return pltpu.make_async_remote_copy(
        src_ref=src, dst_ref=dst, send_sem=send, recv_sem=recv, device_id=where, device_id_type=MESH
    )


def shift(axis, step, size):
    return lax.rem(lax.axis_index(axis) + step + size, size)


def steps_in_plane(nx, ny, cores):
    def hops(d):
        return min(d[0], nx - d[0]) + min(d[1], ny - d[1])

    every = [(i, j, k) for i in range(nx) for j in range(ny) for k in range(cores)]
    return sorted(every[1:], key=lambda d: -hops(d))


def target(d, nx, ny):
    x, y, c = shift("x", d[0], nx), shift("y", d[1], ny), shift("c", d[2], 2)
    chip = x * ny + y
    return {"x": x, "y": y, "c": c}, chip, chip * 2 + c


def rows_of(ref, slot, step, nz):
    part = ref.shape[1] // nz
    return ref.at[slot, pl.ds(pl.multiple_of(shift("z", step, nz) * part, part), part)]


def z_place(step, nz):
    return {"z": shift("z", step, nz)}


class Flight:
    def __init__(self, copies):
        self.copies = copies
        for copy in copies:
            copy.start()

    def recv(self):
        for copy in self.copies:
            copy.wait_recv()

    def send(self):
        for copy in self.copies:
            copy.wait_send()


class Ring:
    def __init__(self, grad, bufs, send, recv, nz):
        self.grad, self.nz, self.s, self.r = grad, nz, send, recv
        self.far, self.src, self.near, self.side = bufs
        self.flights = []

    def go(self, copies):
        self.flights.append(Flight(copies))
        return self.flights[-1]

    def first(self, slot):
        step = -1 if slot == 0 else 1
        self.go([
            remote(rows_of(self.grad, slot, 2, self.nz), self.far.at[slot], self.s.at[0, slot], self.r.at[0, slot], z_place(step, self.nz)),
            remote(rows_of(self.grad, slot, -step, self.nz), self.side.at[slot], self.s.at[1, slot], self.r.at[1, slot], z_place(-step, self.nz)),
        ])

    def second(self):
        for slot in range(2):
            step = -1 if slot == 0 else 1
            self.flights[slot].copies[0].wait_recv()
            mine = rows_of(self.grad, slot, step, self.nz)[...]
            self.src[slot] = (self.far[slot].astype(F32) + mine.astype(F32)).astype(BF16)
            self.go([remote(self.src.at[slot], self.near.at[slot], self.s.at[2, slot], self.r.at[2, slot], z_place(step, self.nz))])

    def finish(self, halves, swap, send, recv):
        ci = lax.axis_index("c")
        half = halves.shape[2]
        for slot in range(2):
            self.flights[slot].copies[1].wait_recv()
            self.flights[2 + slot].recv()
            mine = rows_of(self.grad, slot, 0, self.nz)[...].astype(F32)
            rows = (mine + self.near[slot].astype(F32) + self.side[slot].astype(F32)).astype(BF16)
            low, high = rows[:half], rows[half:]
            halves[ci, slot] = jnp.where(ci == 0, low, high)
            swap[slot] = jnp.where(ci == 0, high, low)
        return self.go([remote(swap, halves.at[ci], send, recv, {"c": 1 - ci})])

    def end(self):
        for flight in self.flights:
            flight.send()


def moved(rows, offset, left):
    window = rows.shape[1]
    bits = jnp.full(rows.shape, offset, jnp.int32)
    for bit in (4, 8, 16, 32, 64):
        rows = jnp.where((bits & bit) != 0, pltpu.roll(rows, window - bit if left else bit, 1), rows)
    return rows


def band_window(blocks, info, j, feat):
    base = info[SLOT_BASE + j]
    raw = jnp.concatenate([blocks[base + i] for i in range(feat // 128 + 1)], axis=1)
    rows = moved(raw, info[SLOT_OFFSET + j], True)[:, :feat]
    lane = lax.broadcasted_iota(jnp.int32, rows.shape, 1)
    return jnp.where(lane < info[SLOT_COLUMNS + j], rows, 0.0)


def normed_tile(blocks, info, j, feat):
    raw = band_window(blocks, info, j, feat)
    counted = jnp.maximum(jnp.full((raw.shape[0], 1), info[SLOT_COLUMNS + j], jnp.int32), 1).astype(F32)
    mean = jnp.sum(raw * raw, axis=1, keepdims=True) / counted
    return (raw * lax.rsqrt(mean + EPSILON)).astype(BF16)


def permutation(rows, frames, bands, to_frames):
    a = lax.broadcasted_iota(jnp.int32, (rows, rows), 0)
    b = lax.broadcasted_iota(jnp.int32, (rows, rows), 1)
    if not to_frames:
        a, b = b, a
    return ((a // bands == b % frames) & (a % bands == b // frames)).astype(F32).astype(BF16)


def gather_bands(src, info, stage):
    for b in range(stage.shape[0]):
        stage[b] = src[info[SLOT + b]]


def scatter_slots(stage, info, dst):
    _, pair, frames, width = dst.shape

    def step(p, carry):
        for s in range(pair):
            j = p * pair + s
            live = jnp.full((frames, width), info[SLOT_COLUMNS + j], jnp.int32) > 0
            dst[p, s] = jnp.where(live, stage[info[SLOT_BAND + j]].astype(F32), 0.0).astype(BF16)
        return carry

    lax.fori_loop(0, dst.shape[0], step, 0, unroll=4)


def attention_forward(tok, info, w_qkv, w_proj, dst, rows_ref, packed, soft_ref, heads_ref, stage):
    bands, frames, width = stage.shape
    rows = bands * frames
    inner = w_proj.shape[0]
    heads = inner // HEAD_DIM
    gather_bands(tok, info, stage)
    tokens32 = dot(permutation(rows, frames, bands, True), stage[...].reshape(rows, width), 1, 0)
    rows_ref[...] = tokens32.astype(BF16)
    inv = lax.rsqrt(jnp.mean(tokens32 * tokens32, axis=1, keepdims=True) + EPSILON)
    packed[...] = dot((tokens32 * inv).astype(BF16), w_qkv[...], 1, 0).astype(BF16)
    row_id = lax.broadcasted_iota(jnp.int32, (BLOCK, BLOCK), 0) // bands
    col_id = lax.broadcasted_iota(jnp.int32, (BLOCK, BLOCK), 1) // bands
    same = row_id == col_id

    def step(i, carry):
        at = pl.ds(pl.multiple_of(i * BLOCK, BLOCK), BLOCK)
        outs = []
        for h in range(heads):
            lo = h * HEAD_DIM
            q = packed[at, lo : lo + HEAD_DIM]
            k = packed[at, inner + lo : inner + lo + HEAD_DIM]
            v = packed[at, 2 * inner + lo : 2 * inner + lo + HEAD_DIM]
            scores = jnp.where(same, dot(q, k, 1, 1) * HEAD_DIM ** (-0.5), -jnp.inf)
            expd = jnp.exp(scores - jnp.max(scores, axis=1, keepdims=True))
            soft = expd / jnp.sum(expd, axis=1, keepdims=True)
            soft_ref[h, at, :] = soft
            outs.append(dot(soft.astype(BF16), v, 1, 0))
        heads_ref[at, :] = jnp.concatenate(outs, axis=1).astype(BF16)
        return carry

    lax.fori_loop(0, rows // BLOCK, step, 0)
    mixed = (rows_ref[...].astype(F32) + dot(heads_ref[...], w_proj[...], 1, 0)).astype(BF16)
    back = dot(permutation(rows, frames, bands, False), mixed, 1, 0).astype(BF16)
    stage[...] = back.reshape(bands, frames, width)
    scatter_slots(stage, info, dst)


def attention_scores_backward(grad, info, w_proj, packed, soft_ref, stage, grads_ref, dheads, dpacked):
    bands, frames, width = stage.shape
    rows = bands * frames
    inner = w_proj.shape[0]
    heads = inner // HEAD_DIM
    gather_bands(grad, info, stage)
    grads_ref[...] = dot(permutation(rows, frames, bands, True), stage[...].reshape(rows, width), 1, 0).astype(BF16)
    dheads[...] = dot(grads_ref[...], w_proj[...], 1, 1).astype(BF16)

    def step(i, carry):
        at = pl.ds(pl.multiple_of(i * BLOCK, BLOCK), BLOCK)
        dq, dk, dv = [], [], []
        for h in range(heads):
            lo = h * HEAD_DIM
            q = packed[at, lo : lo + HEAD_DIM]
            k = packed[at, inner + lo : inner + lo + HEAD_DIM]
            v = packed[at, 2 * inner + lo : 2 * inner + lo + HEAD_DIM]
            g = dheads[at, lo : lo + HEAD_DIM]
            soft = soft_ref[h, at, :]
            p_grad = dot(g, v, 1, 1)
            dv.append(dot(soft.astype(BF16), g, 0, 0))
            around = soft * (p_grad - jnp.sum(p_grad * soft, axis=1, keepdims=True))
            around = (around * HEAD_DIM ** (-0.5)).astype(BF16)
            dq.append(dot(around, k, 1, 0))
            dk.append(dot(around, q, 0, 0))
        dpacked[at, :] = jnp.concatenate(dq + dk + dv, axis=1).astype(BF16)
        return carry

    lax.fori_loop(0, rows // BLOCK, step, 0)


def attention_sums(rows_ref, heads_ref, grads_ref, dpacked, sums):
    pieces, depth, width = sums.shape
    inner = heads_ref.shape[1]
    small = inner // pieces
    tall = depth - small
    across = 3 * inner // width
    proj = dot(heads_ref[...], grads_ref[...], 0, 0).astype(BF16)
    sums[:, tall:, :] = proj.reshape(pieces, small, width)
    tokens32 = rows_ref[...].astype(F32)
    inv = lax.rsqrt(jnp.mean(tokens32 * tokens32, axis=1, keepdims=True) + EPSILON)
    normed = (tokens32 * inv).astype(BF16)
    for j in range(across):
        part = dot(normed, dpacked[:, j * width : (j + 1) * width], 0, 0).astype(BF16)
        for i in range(pieces // across):
            sums[i * across + j, :tall, :] = part[i * tall : (i + 1) * tall, :]


def attention_tokens_backward(info, w_qkv, rows_ref, grads_ref, dpacked, stage, dst):
    bands, frames, width = stage.shape
    rows = bands * frames
    tokens32 = rows_ref[...].astype(F32)
    inv = lax.rsqrt(jnp.mean(tokens32 * tokens32, axis=1, keepdims=True) + EPSILON)
    normed32 = tokens32 * inv
    gn = dot(dpacked[...], w_qkv[...], 1, 1)
    back = grads_ref[...].astype(F32) + inv * (gn - normed32 * jnp.mean(gn * normed32, axis=1, keepdims=True))
    back = dot(permutation(rows, frames, bands, False), back.astype(BF16), 1, 0).astype(BF16)
    stage[...] = back.reshape(bands, frames, width)
    scatter_slots(stage, info, dst)


def mask_assembly(tiles, info, shifted, out):
    parts, frames, cols = out.shape
    feat = tiles.shape[2]
    bands = (shifted.shape[0] - 1) // 3
    lane = lax.broadcasted_iota(jnp.int32, (frames, feat), 1)
    shifted[3 * bands] = jnp.zeros((frames, 128), F32)

    def shift_band(b, carry):
        tile = jnp.where(lane < info[COLUMNS + b], tiles[info[SLOT + b]].astype(F32), 0.0)
        wide = moved(jnp.concatenate([tile, jnp.zeros((frames, 128), F32)], axis=1), info[OFFSET + b], False)
        for m in range(3):
            shifted[3 * b + m] = wide[:, m * 128 : (m + 1) * 128]
        return carry

    lax.fori_loop(0, bands, shift_band, 0, unroll=4)

    def step(p, carry):
        for half in range(cols // 128):
            i = 3 * (p * (cols // 128) + half)
            total = shifted[info[PICK + i]] + shifted[info[PICK + i + 1]] + shifted[info[PICK + i + 2]]
            out[p, :, half * 128 : (half + 1) * 128] = total.astype(BF16)
        return carry

    lax.fori_loop(0, parts, step, 0, unroll=4)


def tail_slot(s, mixed, cots, wh, wo, mask_ref, dmix_ref, gh, go, normed, hidden, dout, dpre):
    peers, _, frames, width = mixed.shape
    feat = cots.shape[3]
    rows = peers * frames
    chunk = min(rows, 256)
    lump = chunk // frames

    def step(i, carry):
        at = pl.ds(pl.multiple_of(i * chunk, chunk), chunk)
        who = pl.ds(i * lump, lump)
        x = mixed[who, s].reshape(chunk, width).astype(F32)
        inv = lax.rsqrt(jnp.mean(x * x, axis=1, keepdims=True) + EPSILON)
        n = x * inv
        nb = n.astype(BF16)
        normed[at, :] = nb
        t = jnp.tanh(dot(nb, wh[s], 1, 0))
        hb = t.astype(BF16)
        hidden[at, :] = hb
        out = dot(hb, wo[s], 1, 0)
        value = out[:, :feat]
        gate = jax.nn.sigmoid(out[:, feat:])
        mask_ref[who, s] = (value * gate).astype(BF16).reshape(lump, frames, feat)
        c = cots[who, s].reshape(chunk, feat).astype(F32)
        cg = c * gate
        g = jnp.concatenate([cg, cg * value * (1.0 - gate)], axis=1).astype(BF16)
        dout[at, :] = g
        gp = (dot(g, wo[s], 1, 1) * (1.0 - t * t)).astype(BF16)
        dpre[at, :] = gp
        gn = dot(gp, wh[s], 1, 1)
        dm = inv * (gn - n * jnp.mean(gn * n, axis=1, keepdims=True))
        dmix_ref[who, s] = dm.astype(BF16).reshape(lump, frames, width)
        return carry

    lax.fori_loop(0, rows // chunk, step, 0)


def tail_weights(s, gh, go, normed, hidden, dout, dpre):
    go[s] = dot(hidden[...], dout[...], 0, 0).astype(BF16)
    gh[s] = dot(normed[...], dpre[...], 0, 0).astype(BF16)


def own_slots(buf, out, first, rows):
    pair = out.shape[0]
    depth = 32

    def part(base):
        def step(i, carry):
            at = pl.ds(pl.multiple_of(i * depth, depth), depth)
            to = pl.ds(pl.multiple_of(first + i * depth, depth), depth)
            for s in range(pair):
                out[s, to, :] = buf[at, base + s, :]
            return carry

        lax.fori_loop(0, rows // depth, step, 0)

    for c in range(2):
        pl.when(lax.axis_index("c") == c)(functools.partial(part, c * pair))


def step_body(nx, ny, nz, names, *refs):
    r = dict(zip(names, refs))
    xi, yi, zi, ci = (lax.axis_index(n) for n in ("x", "y", "z", "c"))
    chips = nx * ny
    me = xi * ny + yi
    who = me * 2 + ci
    info = r["info"]
    other = {"c": 1 - ci}
    every = steps_in_plane(nx, ny, 2)
    alone = steps_in_plane(nx, ny, 1)
    peers, pair, frames, feat = r["normed"].shape

    barrier = pltpu.get_barrier_semaphore()
    for d in every:
        pl.semaphore_signal(barrier, inc=1, device_id=target(d, nx, ny)[0], device_id_type=MESH)
    for k in range(1, nz):
        pl.semaphore_signal(barrier, inc=1, device_id=z_place(k, nz), device_id_type=MESH)
    loads = []
    chunks = {"h": 4, "o": 4}
    for name, count in chunks.items():
        w, buf = r["w" + name + "_hbm"], r["w" + name + "_buf"]
        rows = w.shape[0] // count
        loads.append([
            pltpu.make_async_copy(w.at[pl.ds(i * rows, rows)], buf.at[i % 2], r["load_sem"].at[len(loads), i])
            for i in range(count)
        ])

    def take(index, name):
        copies = loads[index]
        buf, out = r["w" + name + "_buf"], r["w" + name]
        rows = buf.shape[1]
        for i, copy in enumerate(copies):
            copy.wait()
            own_slots(buf.at[i % 2], out, i * rows, rows)
            if i + 2 < len(copies):
                copies[i + 2].start()

    for copies in loads:
        copies[0].start()
        copies[1].start()
    ends = []

    def same_core(src, dst, job):
        out = []
        for k, d in enumerate(alone):
            where, chip, _ = target(d, nx, ny)
            out.append(remote(src.at[chip], dst.at[me], r["chip_s"].at[job, k], r["chip_r"].at[job, k], where))
        ends.append(Flight(out))
        return ends[-1]

    def piece(ref, place, slot=None):
        if len(ref.shape) == 4:
            return ref.at[place] if slot is None else ref.at[place, slot]
        return ref.at[pl.ds(place * pair, pair)] if slot is None else ref.at[place * pair + slot]

    def to_all(src, dst, job, slot=None, group=None):
        out = []
        for k, d in enumerate(every):
            if group is not None and d[0] != group:
                continue
            where, _, peer = target(d, nx, ny)
            a, b = piece(src, peer, slot), piece(dst, who, slot)
            out.append(remote(a, b, r["all_s"].at[job, k], r["all_r"].at[job, k], where))
        ends.append(Flight(out))
        return ends[-1]

    def keep(src, dst, index, job):
        a, b = (src.at[index], dst.at[index]) if src.shape == r["spec"].shape else (piece(src, index), piece(dst, index))
        copy = pltpu.make_async_copy(a, b, r["keep_sem"].at[job])
        copy.start()
        return copy

    pl.semaphore_wait(barrier, len(every) + nz - 1)

    got_spec = same_core(r["spec"], r["spec_rx"], 0)
    got_cot = same_core(r["cot"], r["cot_rx"], 1)
    kept = [keep(r["spec"], r["spec_rx"], me, 0), keep(r["cot"], r["cot_rx"], me, 1)]
    per = r["spec"].shape[2] // 128
    blocks = (r["spec_blocks"], r["cot_blocks"])
    for b in blocks:
        b[chips * per :] = jnp.zeros((b.shape[0] - chips * per, frames, 128), F32)
    take(1, "o")
    for which, (got, rx) in enumerate(((got_spec, r["spec_rx"]), (got_cot, r["cot_rx"]))):
        got.recv()
        kept[which].wait()
        for p in range(chips):
            for i in range(per):
                blocks[which][p * per + i] = rx[p, :, i * 128 : (i + 1) * 128].astype(F32)
        if which:
            break
        got_normed = []
        for group in sorted(range(nx), key=lambda g: -min(g, nx - g)):
            row = shift("x", group, nx) * ny * 2

            def tile(p, carry):
                for s in range(2):
                    r["normed_tx"][row + p, s] = normed_tile(blocks[0], info, (row + p) * 2 + s, feat)
                return carry

            lax.fori_loop(0, ny * 2, tile, 0, unroll=4)
            got_normed.append(to_all(r["normed_tx"], r["normed"], 0, group=group))
        kept.append(keep(r["normed_tx"], r["normed"], who, 2))

    def cot_tile(p, carry):
        for s in range(2):
            r["cots_tx"][p, s] = band_window(blocks[1], info, p * 2 + s, feat).astype(BF16)
        return carry

    lax.fori_loop(0, chips * 2, cot_tile, 0, unroll=2)
    take(0, "h")
    for flight in got_normed:
        flight.recv()
    kept[2].wait()
    for s in range(pair):
        rows = r["normed"][:, s].reshape(peers * frames, feat)
        r["emb_tx"][:, s] = dot(rows, r["w_embed"][s], 1, 0).astype(BF16).reshape(peers, frames, -1)
    got_tokens = to_all(r["emb_tx"], r["tokens"], 1)
    got_cots = to_all(r["cots_tx"], r["cots"], 2)
    kept = [keep(r["emb_tx"], r["tokens"], who, 0), keep(r["cots_tx"], r["cots"], who, 1)]
    got_tokens.recv()
    kept[0].wait()

    attention_forward(
        r["tokens"], info, r["w_qkv"], r["w_proj"], r["mixed_tx"],
        r["rows"], r["packed"], r["soft"], r["heads"], r["stage"],
    )
    got_mixed = [to_all(r["mixed_tx"], r["mixed"], 3 + s, slot=s) for s in range(pair)]
    mixed_kept = keep(r["mixed_tx"], r["mixed"], who, 2)
    got_cots.recv()
    kept[1].wait()
    mixed_kept.wait()

    ring_o = Ring(r["go"], [r["o_" + n] for n in ("far", "src", "near", "side")], r["ring_s"].at[0], r["ring_r"].at[0], nz)
    ring_h = Ring(r["gh"], [r["h_" + n] for n in ("far", "src", "near", "side")], r["ring_s"].at[1], r["ring_r"].at[1], nz)
    ring_e = Ring(r["ge"], [r["e_" + n] for n in ("far", "src", "near", "side")], r["ring_s"].at[2], r["ring_r"].at[2], nz)
    mine = [r["t_normed"], r["t_hidden"], r["t_dout"], r["t_dpre"]]
    got_dmix = []
    for s in range(pair):
        got_mixed[s].recv()
        tail_slot(s, r["mixed"], r["cots"], r["wh"], r["wo"], r["tiles_tx"], r["dmix_tx"], r["gh"], r["go"], *mine)
        got_dmix.append(to_all(r["dmix_tx"], r["dmix"], 5 + s, slot=s))
        tail_weights(s, r["gh"], r["go"], *mine)
        ring_o.first(s)
        ring_h.first(s)
    kept = [keep(r["dmix_tx"], r["dmix"], who, 0), keep(r["tiles_tx"], r["tiles"], who, 1)]
    got_tiles = to_all(r["tiles_tx"], r["tiles"], 7)
    for flight in got_dmix:
        flight.recv()
    kept[0].wait()
    attention_scores_backward(
        r["dmix"], info, r["w_proj"], r["packed"], r["soft"], r["stage"], r["grads"], r["dheads"], r["dpacked"]
    )
    x_ref, o_ref = r["sums"], r["totals"]
    attention_sums(r["rows"], r["heads"], r["grads"], r["dpacked"], x_ref)

    first = []
    for k, d in enumerate(alone + [(0, 0, 0)]):
        chip = target(d, nx, ny)[1]
        first.append(remote(x_ref.at[(1 - ci) * chips + chip], r["pair"].at[chip], r["pair_s"].at[0, k], r["pair_r"].at[0, k], other))
    ends.append(Flight(first))
    ring_o.second()
    ring_h.second()
    attention_tokens_backward(info, r["w_qkv"], r["rows"], r["grads"], r["dpacked"], r["stage"], r["dtok_tx"])
    landed, part = r["landed"], r["part"]
    to_chips = []
    for k, d in enumerate(alone + [(0, 0, 0)]):
        where, chip, _ = target(d, nx, ny)
        first[k].wait_recv()
        summed = (x_ref[ci * chips + chip].astype(F32) + r["pair"][chip].astype(F32)).astype(BF16)
        if k < len(alone):
            part[chip] = summed
            to_chips.append(Flight([remote(part.at[chip], landed.at[me], r["chip_s"].at[2, k], r["chip_r"].at[2, k], where)]))
        else:
            landed[me] = summed
    ends.extend(to_chips)
    got_dtok = to_all(r["dtok_tx"], r["dtok"], 8)
    kept.append(keep(r["dtok_tx"], r["dtok"], who, 2))
    got_tiles.recv()
    kept[1].wait()
    mask_assembly(r["tiles"], info, r["shifted"], r["mask_tx"])
    got_mask = same_core(r["mask_tx"], r["mask"], 3)
    kept.append(keep(r["mask_tx"], r["mask"], me, 3))
    for flight in to_chips:
        flight.recv()
    total = landed[0].astype(F32)
    for q in range(1, chips):
        total += landed[q].astype(F32)
    deep, final = r["deep"], r["final"]
    r["chip_sum"][...] = total.astype(BF16)
    deep[zi] = total.astype(BF16)
    across = Flight([
        remote(r["chip_sum"], deep.at[zi], r["deep_s"].at[k], r["deep_r"].at[k], z_place(k, nz)) for k in range(1, nz)
    ])
    ends.append(across)
    across.recv()
    total = deep[0].astype(F32)
    for q in range(1, nz):
        total += deep[q].astype(F32)
    final[...] = total.astype(BF16)
    o_ref[ci * chips + me] = total.astype(BF16)
    back = []
    for k, d in enumerate(alone):
        back.append(remote(final, o_ref.at[ci * chips + me], r["chip_s"].at[4, k], r["chip_r"].at[4, k], target(d, nx, ny)[0]))
    ends.append(Flight(back))
    shared = [Flight([remote(final, o_ref.at[ci * chips + me], r["pair_s"].at[1, len(alone)], r["pair_r"].at[1, len(alone)], other)])]

    got_dtok.recv()
    kept[2].wait()
    for s in range(pair):
        left = r["normed"][:, s].reshape(peers * frames, feat)
        right = r["dtok"][:, s].reshape(peers * frames, r["dtok"].shape[3])
        r["ge"][s] = dot(left, right, 0, 0).astype(BF16)
    for s in range(pair):
        ring_e.first(s)
    swaps = [
        ring_o.finish(r["o_half"], r["o_swap"], r["swap_s"].at[0], r["swap_r"].at[0]),
        ring_h.finish(r["h_half"], r["h_swap"], r["swap_s"].at[1], r["swap_r"].at[1]),
    ]
    ring_e.second()
    swaps.append(ring_e.finish(r["e_half"], r["e_swap"], r["swap_s"].at[2], r["swap_r"].at[2]))
    for k, d in enumerate(alone):
        back[k].wait_recv()
        q = ci * chips + target((nx - d[0], ny - d[1], 0), nx, ny)[1]
        shared.append(Flight([remote(o_ref.at[q], o_ref.at[q], r["pair_s"].at[1, k], r["pair_r"].at[1, k], other)]))
    for swap in swaps:
        swap.recv()
    got_mask.recv()
    kept[3].wait()
    for flight in shared:
        flight.recv()
    for flight in ends + shared:
        flight.send()
    for ring in (ring_o, ring_h, ring_e):
        ring.end()
    unpack(o_ref, r["grad_qkv"], r["grad_proj"])


def unpack(sums, qkv, proj):
    pieces, depth, width = sums.shape
    small = proj.shape[0] // pieces
    tall = depth - small
    across = qkv.shape[1] // width
    proj[...] = sums[:, tall:, :].astype(F32).reshape(proj.shape)
    for i in range(pieces // across):
        for j in range(across):
            qkv[i * tall : (i + 1) * tall, j * width : (j + 1) * width] = sums[i * across + j, :tall, :].astype(F32)


def train_step(sizes, info, spec, cot, w_embed, w_qkv, w_proj, w_hidden, w_out):
    nx, ny, nz = sizes
    chips, frames, cols = spec.shape
    peers = 2 * chips
    pair, feat, width = w_embed.shape
    hid, out_cols = w_out.shape[0], w_out.shape[2]
    inner = w_proj.shape[0]
    bands = TABLE // 2
    rows = bands * frames
    many = peers * frames
    pieces = peers
    depth = 4 * inner // pieces
    dma = pltpu.SemaphoreType.DMA

    def vm(*shape):
        return pltpu.VMEM(shape, BF16)

    ins = {
        "info": (info, SMEM), "spec": (spec, VMEM), "cot": (cot, VMEM), "w_embed": (w_embed, VMEM),
        "w_qkv": (w_qkv, VMEM), "w_proj": (w_proj, VMEM), "wh_hbm": (w_hidden, ANY), "wo_hbm": (w_out, ANY),
    }
    dims = {"o": (hid, out_cols), "h": (width, hid), "e": (feat, width)}
    outs = {
        "mask": jax.ShapeDtypeStruct(spec.shape, BF16),
        "grad_qkv": jax.ShapeDtypeStruct(w_qkv.shape, F32),
        "grad_proj": jax.ShapeDtypeStruct(w_proj.shape, F32),
    }
    for n, (a, b) in dims.items():
        outs[n + "_half"] = jax.ShapeDtypeStruct((2, pair, a // nz // 2, b), BF16)
    scratch = {
        "spec_rx": vm(*spec.shape), "cot_rx": vm(*spec.shape),
        "spec_blocks": pltpu.VMEM((chips * cols // 128 + 3, frames, 128), F32),
        "cot_blocks": pltpu.VMEM((chips * cols // 128 + 3, frames, 128), F32),
        "shifted": pltpu.VMEM((3 * bands + 1, frames, 128), F32),
        "wh_buf": vm(2, width // 4, *w_hidden.shape[1:]), "wo_buf": vm(2, hid // 4, *w_out.shape[1:]),
        "wh": vm(pair, width, hid), "wo": vm(pair, hid, out_cols),
        "normed_tx": vm(peers, pair, frames, feat), "normed": vm(peers, pair, frames, feat),
        "cots_tx": vm(peers, pair, frames, feat), "cots": vm(peers, pair, frames, feat),
        "tiles_tx": vm(peers, pair, frames, feat), "tiles": vm(peers * pair, frames, feat),
        "mask_tx": vm(*spec.shape),
        "rows": vm(rows, width), "packed": vm(rows, 3 * inner), "heads": vm(rows, inner),
        "soft": pltpu.VMEM((inner // HEAD_DIM, rows, BLOCK), F32),
        "stage": vm(bands, frames, width), "grads": vm(rows, width), "dheads": vm(rows, inner), "dpacked": vm(rows, 3 * inner),
        "t_normed": vm(many, width), "t_hidden": vm(many, hid), "t_dout": vm(many, out_cols), "t_dpre": vm(many, hid),
        "go": vm(pair, hid, out_cols), "gh": vm(pair, width, hid), "ge": vm(pair, feat, width),
        "sums": vm(pieces, depth, width), "totals": vm(pieces, depth, width),
        "pair": vm(chips, depth, width), "part": vm(chips, depth, width), "landed": vm(chips, depth, width),
        "chip_sum": vm(depth, width), "deep": vm(nz, depth, width), "final": vm(depth, width),
    }
    for n in ("emb_tx", "mixed_tx", "mixed", "dmix_tx", "dtok_tx", "dtok"):
        scratch[n] = vm(peers, pair, frames, width)
    for n in ("tokens", "dmix"):
        scratch[n] = vm(peers * pair, frames, width)
    for n, (a, b) in dims.items():
        for kind in ("far", "src", "near", "side"):
            scratch[n + "_" + kind] = vm(pair, a // nz, b)
        scratch[n + "_swap"] = vm(pair, a // nz // 2, b)
    for n, shape in {
        "load_sem": (2, 4), "keep_sem": (4,), "chip_s": (5, chips), "chip_r": (5, chips), "all_s": (9, peers), "all_r": (9, peers),
        "pair_s": (2, chips), "pair_r": (2, chips), "deep_s": (nz,), "deep_r": (nz,), "ring_s": (3, 3, 2), "ring_r": (3, 3, 2),
        "swap_s": (3,), "swap_r": (3,),
    }.items():
        scratch[n] = dma(shape)
    names = list(ins) + list(outs) + list(scratch)
    results = pl.pallas_call(
        functools.partial(step_body, nx, ny, nz, names),
        out_shape=list(outs.values()),
        in_specs=[spec for _, spec in ins.values()],
        out_specs=[VMEM] * len(outs),
        scratch_shapes=list(scratch.values()),
        compiler_params=pltpu.CompilerParams(collective_id=0, has_side_effects=True, vmem_limit_bytes=63 * MIB),
    )(*[array for array, _ in ins.values()])
    return dict(zip(outs, results))


def interleaved(halves):
    return halves.reshape(-1, *halves.shape[2:]).transpose(1, 0, 2)


def per_device(spec, cotangent, widths, band_group, w_embed, w_qkv, w_proj, w_hidden, w_out):
    frames, cols = spec.shape
    slot_count = w_embed.shape[1]
    sizes = tuple(lax.axis_size(n) for n in ("x", "y", "z"))
    groups = sizes[0] * sizes[1]
    pair = slot_count // 2
    each = frames // groups
    own = lax.dynamic_slice_in_dim(w_embed, lax.axis_index("c") * pair, pair, 1).transpose(1, 0, 2)
    info = tables(widths, band_group, groups, slot_count, groups * cols // 128)
    out = train_step(
        sizes, info, spec.reshape(groups, each, cols), cotangent.reshape(groups, each, cols),
        own, w_qkv, w_proj, w_hidden, w_out,
    )
    return (
        out["mask"].reshape(frames, cols),
        interleaved(out["e_half"]),
        out["grad_qkv"],
        out["grad_proj"],
        interleaved(out["h_half"]),
        interleaved(out["o_half"]),
    )


def solution(mesh):
    split = Mesh(mesh.devices.reshape(4, 4, 4, 2), ("x", "y", "z", "c"))
    band = ("x", "y")
    tm = ("z", "c")
    placed = (
        P(tm, band),
        P(tm, band),
        P(),
        P(),
        P(None, band, None),
        P(),
        P(),
        P(None, band, None),
        P(None, band, None),
    )
    return jax.shard_map(
        per_device,
        mesh=split,
        in_specs=placed,
        out_specs=(
            P(tm, band),
            P(tm, band, None),
            P(),
            P(),
            P(tm, band, None),
            P(tm, band, None),
        ),
        check_vma=False,
    )
```
